32 devices in a mesh: head: 8 (over z, x), client: 4 (over y, core).
Axes of the slice: x: 2, y: 2, z: 4, core: 2. Of those that a mesh axis runs over, the one named last changes fastest.
Arguments:
- client_ids: int32 [32], replicated, may hold values from 0 to 127, as said below
- client_table: bfloat16 [128, 256], replicated, may hold values from -6 to 6
- in_weight: bfloat16 [256, 4096], P(None, 'client'), may hold values from -0.375 to 0.375
- in_bias: float32 [4096], P('client'), may hold values from -3 to 3
- head_weight: bfloat16 [4096, 131072], P('client', 'head'), may hold values from -0.09375 to 0.09375
- tokens: int32 [32, 256], P(('head', 'client')), may hold values from 0 to 255
- labels: int32 [32, 256], P(('head', 'client')), may hold values from 0 to 255
- byte_table: bfloat16 [256, 4096], P(None, 'client'), may hold values from -5.5 to 6.7
- out_table: bfloat16 [256, 4096], P(None, 'client'), may hold values from -5.625 to 5.625
Outputs:
- head_grad: bfloat16 [4096, 131072], P('client', 'head')
- in_grad: float32 [256, 4096], P(None, 'client')
- losses: float32 [32], P(('head', 'client'))
The draws below stay inside these ranges and needn't reach their ends.
Inputs may be any that keep to these rules, and one draw needn't show every extreme that they name: `client_ids`: distinct population indices.
All inputs are finite; a program needn't handle non-finite values.
Results may differ from the reference program's by a relative error of at most 0.0085.
Values may be sent and summed in bfloat16 or wider, within the bound.
No kernel may reach another device: no remote copies, remote signals or barrier semaphores. Data moves between devices by JAX's collectives and lax.ppermute only.
A program may use at most 128 MiB of HBM per device.

```python
import jax
import jax.numpy as jnp
from jax import lax

H = 4096
E = 256
D = 4096
VOCAB = 256
SEQ = 256
CLIENTS = 32
NPOP = 128
P_SIZE = 131072


def draw_client_ids(key, part):
    return jax.random.permutation(key, NPOP)[:CLIENTS].astype(jnp.int32)


def table_parts(key):
    noise_key = jax.random.fold_in(jax.random.fold_in(key, 7), 0)
    values = jnp.clip(jax.random.normal(noise_key, (VOCAB, D), jnp.float32), -5.5, 5.5)
    return values


def draw_byte_table(key, part):
    values = table_parts(key)
    return values.astype(jnp.bfloat16)


def draw_out_table(key, part):
    values = jnp.clip(jax.random.normal(jax.random.fold_in(key, 11), (VOCAB, D), jnp.float32), -5.5, 5.5)
    return values.astype(jnp.bfloat16)


def touch_ends(entries, key, low, largest):
    spot = [jax.random.randint(jax.random.fold_in(key, axis), (), 0, length) for axis, length in enumerate(entries.shape)]
    widest = entries.shape.index(max(entries.shape))
    next_to = spot[:widest] + [(spot[widest] + 1) % entries.shape[widest]] + spot[widest + 1:]
    return entries.at[tuple(spot)].set(low).at[tuple(next_to)].set(largest)


def level_of(stream_key, dims, pieces, low, top_value):
    level, own = 1.0, jax.random.fold_in(stream_key, 6)
    for position, shards_of in pieces:
        heights = jnp.exp(jax.random.uniform(jax.random.fold_in(own, position), (shards_of,), jnp.float32, low / len(pieces), top_value / len(pieces)))
        level = level * jnp.repeat(heights, dims[position] // shards_of).reshape([-1 if axis == position else 1 for axis in range(len(dims))])
    return level


def scatter_about(own_key, dims, scale, limit, shards=(), held_as=jnp.bfloat16):
    loudness = level_of(own_key, dims, shards, -0.22, 0.18) if shards else 1.0
    entries = jax.random.normal(own_key, dims, jnp.float32) * scale * loudness
    return jnp.minimum(jnp.maximum(entries, -limit), limit).astype(held_as)


def setup_inputs(seed: int = 0) -> dict:
    keys = jax.random.split(jax.random.key(seed), 10)
    client_ids = draw_client_ids(jax.random.fold_in(keys[9], 71), 0)
    client_table = scatter_about(keys[1], (NPOP, E), 1.0, 6.0)
    in_weight = scatter_about(keys[2], (E, H), E ** -0.5, 0.375, ((1, 4),))
    in_bias = scatter_about(keys[3], (H,), 0.5, 3.0, ((0, 4),), jnp.float32)
    head_weight = scatter_about(keys[4], (H, P_SIZE), H ** -0.5, 0.09375, ((0, 4), (1, 8)))
    tokens = touch_ends(jax.random.randint(keys[5], (CLIENTS, SEQ), 0, VOCAB), jax.random.fold_in(keys[5], 1), 0, VOCAB - 1).astype(jnp.int32)
    labels = touch_ends(jax.random.randint(keys[6], (CLIENTS, SEQ), 0, VOCAB), jax.random.fold_in(keys[6], 1), 0, VOCAB - 1).astype(jnp.int32)
    byte_table = draw_byte_table(jax.random.fold_in(keys[9], 71), 0)
    out_table = draw_out_table(jax.random.fold_in(keys[9], 71), 0)
    return dict(client_ids=client_ids, client_table=client_table, in_weight=in_weight, in_bias=in_bias, head_weight=head_weight, tokens=tokens, labels=labels, byte_table=byte_table, out_table=out_table)


EPSILON = 1e-06
learn_rate = 0.1

def client_loss(factor_a, factor_b, inputs, label_row, out_table):
    depth = factor_a.shape[0]
    rank_size = factor_a.shape[1]
    normed_in = inputs * lax.rsqrt(lax.optimization_barrier(jnp.mean(inputs * inputs, -1, keepdims=True)) + EPSILON)
    low_rank = jnp.dot(normed_in, factor_a, precision=lax.Precision.HIGHEST)
    adapted = inputs + jnp.dot(low_rank, factor_b, precision=lax.Precision.HIGHEST) / jnp.sqrt(jnp.float32(depth * rank_size))
    normed = (adapted * lax.rsqrt(lax.optimization_barrier(jnp.mean(adapted * adapted, -1, keepdims=True)) + EPSILON)).astype(jnp.bfloat16)
    logits = lax.dot_general(normed, out_table, (((1,), (1,)), ((), ())), preferred_element_type=jnp.float32)
    logits = logits * (4.0 / jnp.sqrt(jnp.float32(depth)))
    log_total = jax.nn.logsumexp(logits, -1)
    vocab_ids = lax.broadcasted_iota(jnp.int32, logits.shape, 1)
    picked = lax.optimization_barrier(jnp.sum(jnp.where(vocab_ids == label_row[:, None], logits, 0.0), -1))
    return jnp.sum(log_total - picked)

def train_client(factor_row, token_row, label_row, byte_table, out_table):
    depth = byte_table.shape[1]
    split_at = factor_row.shape[0] // 2
    rank_size = split_at // depth
    start_a = factor_row[:split_at].reshape(depth, rank_size).astype(jnp.float32)
    start_b = factor_row[split_at:].reshape(rank_size, depth).astype(jnp.float32)
    onehot = (token_row[:, None] == lax.broadcasted_iota(jnp.int32, (token_row.shape[0], byte_table.shape[0]), 1)).astype(jnp.bfloat16)
    inputs = jnp.dot(onehot, byte_table, preferred_element_type=jnp.float32)
    loss_grad = jax.value_and_grad(client_loss, argnums=(0, 1))
    first_loss, (grad_a, grad_b) = loss_grad(start_a, start_b, inputs, label_row, out_table)
    middle_a = start_a - learn_rate * grad_a
    middle_b = start_b - learn_rate * grad_b
    second_loss, (grad_a, grad_b) = loss_grad(middle_a, middle_b, inputs, label_row, out_table)
    final_a = middle_a - learn_rate * grad_a
    final_b = middle_b - learn_rate * grad_b
    deltas = jnp.concatenate([(final_a - start_a).reshape(-1), (final_b - start_b).reshape(-1)]).astype(jnp.bfloat16)
    return (deltas, first_loss / token_row.shape[0])

def reference(client_ids, client_table, in_weight, in_bias, head_weight, tokens, labels, byte_table, out_table):
    chosen = client_table[client_ids]
    preact = jnp.dot(chosen, in_weight, preferred_element_type=jnp.float32) + in_bias
    hidden = jnp.maximum(preact, 0.0).astype(jnp.bfloat16)
    factors = jnp.dot(hidden, head_weight, preferred_element_type=jnp.float32).astype(jnp.bfloat16)
    blocks = CLIENTS // 8

    def run_block(record):
        return jax.vmap(lambda fac, tok, lab: train_client(fac, tok, lab, byte_table, out_table))(record[0], record[1], record[2])
    deltas, losses = lax.map(run_block, (factors.reshape(blocks, 8, -1), tokens.reshape(blocks, 8, -1), labels.reshape(blocks, 8, -1)))
    deltas = deltas.reshape(CLIENTS, -1)
    losses = losses.reshape(CLIENTS)
    head_grad = lax.dot_general(hidden, deltas, (((0,), (0,)), ((), ())), preferred_element_type=jnp.float32).astype(jnp.bfloat16)
    hidden_back = lax.dot_general(deltas, head_weight, (((1,), (1,)), ((), ())), preferred_element_type=jnp.float32)
    masked = jnp.where(preact > 0, hidden_back, 0.0)
    in_grad = lax.dot_general(chosen.astype(jnp.float32), masked, (((0,), (0,)), ((), ())), precision=lax.Precision.HIGHEST)
    return (head_grad, in_grad, losses)
```

```python
import functools

import jax
import jax.numpy as jnp
from jax import lax
from jax.experimental import pallas as pl
from jax.experimental.pallas import tpu as pltpu
from jax.sharding import PartitionSpec as P

EPSILON = 1e-06
learn_rate = 0.1
F32 = jnp.float32
BF16 = jnp.bfloat16
LANES = 128
HIGH = lax.Precision.HIGHEST


def dot(a, b, contract, precision=None):
    return lax.dot_general(a, b, ((contract[0], contract[1]), ((), ())), precision=precision, preferred_element_type=F32)


NN = ((1,), (0,))
NT = ((1,), (1,))
TN = ((0,), (0,))


def bits_of(count):
    return count.bit_length() - 1


def offset_of(position, count):
    bits = bits_of(count)
    return sum(((position >> (bits - 1 - bit)) & 1) << bit for bit in range(bits))


def small(a, b):
    return sum(a[:, k : k + 1] * b[k : k + 1, :] for k in range(a.shape[1]))


def span(index, width):
    return pl.ds(pl.multiple_of(index * width, LANES), width)


def forward_kernel(head_count, group_count, width, place, ids, table, in_w, in_b, w, keep, send, hidden_t, preact_out, chosen_t, held, hidden, sems):
    slots = held.shape[0]
    rows = keep.shape[0] * 2
    blocks = w.shape[1] // width

    def copy(index):
        return pltpu.make_async_copy(w.at[:, span(index, width)], held.at[index % slots], sems.at[index % slots])

    @pl.loop(0, slots)
    def _(index):
        copy(index).start()

    row = lax.broadcasted_iota(jnp.int32, (rows, rows), 0)
    column = lax.broadcasted_iota(jnp.int32, (rows, rows), 1)
    position = row // head_count
    bits = bits_of(group_count)
    offset = jnp.zeros_like(position)
    for bit in range(bits):
        offset = offset + (((position >> (bits - 1 - bit)) & 1) << bit)
    slot = (row % head_count) * group_count + jnp.bitwise_xor(offset, place[0])
    picked = jnp.sum(jnp.where(column == slot, ids[...], 0), axis=1, keepdims=True)
    people = table.shape[0]
    onehot = (lax.broadcasted_iota(jnp.int32, (rows, people), 1) == picked).astype(F32).astype(BF16)
    chosen = dot(onehot, table[...], NN)
    preact = dot(chosen.astype(BF16), in_w[...], NN) + in_b[...]
    value = jnp.maximum(preact, 0.0)
    hidden[...] = value.astype(BF16)
    hidden_t[...] = value.T.astype(BF16)
    chosen_t[...] = chosen.T.astype(BF16)
    preact_out[...] = preact

    @pl.loop(0, blocks)
    def _(index):
        copy(index).wait()
        part = dot(hidden[...], held[index % slots], NN)
        keep[:, span(index, width)] = part[: rows // 2]
        send[:, span(index, width)] = part[rows // 2 :].astype(BF16)

        @pl.when(index + slots < blocks)
        def _():
            copy(index + slots).start()


def forward(place, ids, table, in_w, in_b, w, head_count, group_count):
    rows = ids.shape[1]
    depth, columns = w.shape
    width = min(1024, columns)
    whole = pl.BlockSpec(memory_space=pltpu.VMEM)
    shapes = [
        ((rows // 2, columns), F32),
        ((rows // 2, columns), BF16),
        ((depth, rows), BF16),
        ((rows, depth), F32),
        ((table.shape[1], rows), BF16),
    ]
    slots = min(6, columns // width)
    return pl.pallas_call(
        functools.partial(forward_kernel, head_count, group_count, width),
        in_specs=[pl.BlockSpec(memory_space=pltpu.SMEM)] + [whole] * 4 + [pl.BlockSpec(memory_space=pltpu.HBM)],
        out_specs=[whole] * len(shapes),
        out_shape=[jax.ShapeDtypeStruct(*shape) for shape in shapes],
        scratch_shapes=[pltpu.VMEM((slots, depth, width), BF16), pltpu.VMEM((rows, depth), BF16), pltpu.SemaphoreType.DMA((slots,))],
        compiler_params=pltpu.CompilerParams(vmem_limit_bytes=40 * 1024 * 1024),
        cost_estimate=pl.CostEstimate(flops=32 * rows * depth * columns, bytes_accessed=2 * depth * columns, transcendentals=0),
        name="factors",
    )(place, ids, table, in_w, in_b, w)


def prepare_kernel(group_count, step, place, tokens, *refs):
    byte_parts, out_parts = refs[:group_count], refs[group_count : 2 * group_count]
    byte_full, out_full, byte_mixed, logit_gram, grams, normed_gram, inverse, squares = refs[2 * group_count :]
    vocab, width = byte_parts[0].shape
    depth = byte_full.shape[1]
    inner = width // step
    pair = min(2, step)
    gap = lax.broadcasted_iota(jnp.int32, (width, inner), 0) - step * lax.broadcasted_iota(jnp.int32, (width, inner), 1)
    byte_gram = jnp.zeros((vocab, vocab), F32)
    cross = jnp.zeros((vocab, vocab), F32)
    own_gram = jnp.zeros((vocab, vocab), F32)
    for position in range(group_count):
        start = jnp.bitwise_xor(place[0], offset_of(position, group_count))
        byte_part, out_part = byte_parts[position][...], out_parts[position][...]
        byte_full[:, pl.ds(pl.multiple_of(start * width, LANES), width)] = byte_part
        out_full[:, pl.ds(pl.multiple_of(start * width, LANES), width)] = out_part
        byte_gram += dot(byte_part, byte_part, NT)
        cross += dot(out_part, byte_part, NT)
        own_gram += dot(out_part, out_part, NT)
    for first in range(0, step, pair):
        mixer = jnp.concatenate([jnp.where(gap == first + k, 1.0, 0.0) for k in range(pair)], axis=1).astype(BF16)
        for position in range(group_count):
            start = jnp.bitwise_xor(place[0], offset_of(position, group_count))
            mixed = dot(byte_parts[position][...], mixer, NN).astype(BF16)
            for k in range(pair):
                at = pl.multiple_of((first + k) * (depth // step) + start * inner, LANES)
                byte_mixed[:, pl.ds(at, inner)] = mixed[:, k * inner : (k + 1) * inner]
    count = tokens.shape[1]
    onehot = (lax.broadcasted_iota(jnp.int32, (vocab, count), 0) == tokens[...]).astype(F32)
    logit = dot(cross, onehot, NN, HIGH)
    logit_gram[...] = logit
    half = dot(byte_gram, onehot, NN, HIGH)
    total = jnp.sum(onehot * half, axis=0, keepdims=True)
    both = dot(onehot, half, TN, HIGH)
    scale = lax.rsqrt(total / depth + EPSILON)
    eye = lax.broadcasted_iota(jnp.int32, (count, count), 0) == lax.broadcasted_iota(jnp.int32, (count, count), 1)
    down = jnp.sum(jnp.where(eye, scale, 0.0), axis=1, keepdims=True)
    grams[:vocab, :vocab] = own_gram
    grams[:vocab, vocab:] = logit
    grams[vocab:, :vocab] = logit.T
    grams[vocab:, vocab:] = both
    normed_gram[...] = both * scale * down
    inverse[...] = scale
    squares[...] = total


def prepare(place, tokens, byte_parts, out_parts, step):
    group_count = len(byte_parts)
    vocab, width = byte_parts[0].shape
    count = tokens.shape[1]
    depth = width * group_count
    whole = pl.BlockSpec(memory_space=pltpu.VMEM)
    shapes = [
        ((vocab, depth), BF16),
        ((vocab, depth), BF16),
        ((vocab, depth), BF16),
        ((vocab, count), F32),
        ((vocab + count, vocab + count), F32),
        ((count, count), F32),
        ((1, count), F32),
        ((1, count), F32),
    ]
    return pl.pallas_call(
        functools.partial(prepare_kernel, group_count, step),
        in_specs=[pl.BlockSpec(memory_space=pltpu.SMEM)] + [whole] * (1 + 2 * group_count),
        out_specs=[whole] * len(shapes),
        out_shape=[jax.ShapeDtypeStruct(*shape) for shape in shapes],
        compiler_params=pltpu.CompilerParams(vmem_limit_bytes=16 * 1024 * 1024),
        cost_estimate=pl.CostEstimate(flops=2**31, bytes_accessed=2**23, transcendentals=0),
        name="prepare",
    )(place, tokens, *byte_parts, *out_parts)


def train_kernel(
    rank,
    owned,
    tokens,
    labels,
    byte_full,
    out_full,
    byte_mixed,
    logit_gram,
    grams,
    normed_gram,
    inverse,
    squares,
    deltas,
    loss_out,
    work,
):
    vocab, depth = byte_full.shape
    count = tokens.shape[1]
    step = LANES // rank
    rows = depth * rank // LANES
    inner = depth // step
    chunks = depth // LANES
    onehot = (lax.broadcasted_iota(jnp.int32, (vocab, count), 0) == tokens[...]).astype(F32)
    label = (lax.broadcasted_iota(jnp.int32, (vocab, count), 0) == labels[...]).astype(F32)
    scale = inverse[...]
    a_t = owned[:rows, :].astype(F32).T.astype(BF16)
    table_a = jnp.zeros((rank, vocab), F32)
    for j in range(step):
        table_a += dot(a_t[j * rank : (j + 1) * rank, :], byte_mixed[:, j * inner : (j + 1) * inner], NT)
    work[...] = owned[rows:, :].astype(F32)
    b = jnp.concatenate([work[pl.ds(k, rank, stride=chunks), :] for k in range(chunks)], axis=1).astype(BF16)
    out_b = dot(b, out_full[...], NT)
    byte_b = dot(b, byte_full[...], NT)
    gram_b = dot(b, b, NT)
    low = dot(table_a, onehot, NN, HIGH) * scale
    in_b = dot(byte_b, onehot, NN, HIGH)
    s = 1.0 / (depth * rank) ** 0.5
    c = 4.0 / depth**0.5

    def one_step(low, both_b, gram_b):
        out_b, in_b = both_b[:, :vocab], both_b[:, vocab:]
        low_gram = small(gram_b, low)
        mean = (squares[...] + jnp.sum(low * (2.0 * s * in_b + (s * s) * low_gram), axis=0, keepdims=True)) / depth
        r = lax.rsqrt(jnp.maximum(mean, 0.0) + EPSILON)
        raw = logit_gram[...] + s * dot(out_b, low, TN, HIGH)
        logits = raw * (c * r)
        top = jnp.max(logits, axis=0, keepdims=True)
        grown = jnp.exp(logits - top)
        total = jnp.sum(grown, axis=0, keepdims=True)
        loss = jnp.log(total) + top - jnp.sum(label * logits, axis=0, keepdims=True)
        error = grown / total - label
        k = (c / depth) * (r * r * r) * jnp.sum(error * raw, axis=0, keepdims=True)
        error = error * (c * r)
        d_low = s * (dot(out_b, error, NN, HIGH) - k * (in_b + s * low_gram))
        kept = k * low
        on_both = rate * jnp.concatenate([-dot(low, error, NT, HIGH), kept], axis=1)
        return loss, d_low, on_both, (rate * s) * dot(kept, low, NT, HIGH)

    rate = learn_rate * s
    both_b = jnp.concatenate([out_b, in_b], axis=1)
    loss, d_low, on_both, more = one_step(low, both_b, gram_b)
    low_1 = low - learn_rate * dot(d_low, normed_gram[...], NN, HIGH)
    both_b1 = both_b + small(more, both_b) + dot(on_both, grams[...], NN, HIGH)
    gram_1 = gram_b + small(more, gram_b) + dot(on_both, both_b, NT, HIGH)
    gram_b1 = gram_1 + small(gram_1, more.T) + dot(both_b1, on_both, NT, HIGH)
    _, d_low1, on_both1, more1 = one_step(low_1, both_b1, gram_b1)
    total_b = more + more1 + small(more1, more)
    total_both = on_both + on_both1 + small(more1, on_both)
    total_out, total_in = total_both[:, :vocab], total_both[:, vocab:]
    on_byte = dot(total_in, onehot, NT, HIGH)
    on_a = dot((-learn_rate) * scale * (d_low + d_low1), onehot, NT, HIGH).astype(BF16)
    pieces = [dot(on_a, byte_mixed[:, j * inner : (j + 1) * inner], NN) for j in range(step)]
    deltas[:rows, :] = jnp.concatenate(pieces, axis=0).T.astype(BF16)
    delta_b = dot(total_b.astype(BF16), b, NN) + dot(total_out.astype(BF16), out_full[...], NN) + dot(on_byte.astype(BF16), byte_full[...], NN)
    for k in range(chunks):
        work[pl.ds(k, rank, stride=chunks), :] = delta_b[:, k * LANES : (k + 1) * LANES]
    deltas[rows:, :] = work[...].astype(BF16)
    loss_out[...] = jnp.broadcast_to(jnp.sum(loss, axis=1, keepdims=True) / count, loss_out.shape)


def train(rank, owned, tokens, labels, prepared):
    whole = pl.BlockSpec(memory_space=pltpu.VMEM)
    return pl.pallas_call(
        functools.partial(train_kernel, rank),
        in_specs=[whole] * (3 + len(prepared)),
        out_specs=[whole, whole],
        out_shape=[jax.ShapeDtypeStruct(owned.shape, BF16), jax.ShapeDtypeStruct((1, LANES), F32)],
        scratch_shapes=[pltpu.VMEM((owned.shape[0] // 2, LANES), F32)],
        compiler_params=pltpu.CompilerParams(vmem_limit_bytes=16 * 1024 * 1024),
        cost_estimate=pl.CostEstimate(flops=2**31, bytes_accessed=2**23, transcendentals=2**17),
        name="train",
    )(owned, tokens, labels, *prepared)


def stacked(parts):
    return jnp.concatenate([part[...].astype(F32) for part in parts], axis=0).astype(BF16)


def back_kernel(width, w, *refs):
    parts, out, held, sems = refs[:-3], refs[-3], refs[-2], refs[-1]
    slots = held.shape[0]
    blocks = w.shape[1] // width

    def copy(index):
        return pltpu.make_async_copy(w.at[:, span(index, width)], held.at[index % slots], sems.at[index % slots])

    @pl.loop(0, slots)
    def _(index):
        copy(index).start()

    out[...] = jnp.zeros_like(out)

    @pl.loop(0, blocks)
    def _(index):
        piece = stacked([part.at[:, span(index, width)] for part in parts])
        copy(index).wait()
        out[...] += dot(piece, held[index % slots], NT)

        @pl.when(index + slots < blocks)
        def _():
            copy(index + slots).start()


def back(w, parts):
    depth, columns = w.shape
    rows = sum(part.shape[0] for part in parts)
    width = min(1024, columns)
    slots = min(6, columns // width)
    whole = pl.BlockSpec(memory_space=pltpu.VMEM)
    return pl.pallas_call(
        functools.partial(back_kernel, width),
        in_specs=[pl.BlockSpec(memory_space=pltpu.HBM)] + [whole] * len(parts),
        out_specs=whole,
        out_shape=jax.ShapeDtypeStruct((rows, depth), F32),
        scratch_shapes=[pltpu.VMEM((slots, depth, width), BF16), pltpu.SemaphoreType.DMA((slots,))],
        compiler_params=pltpu.CompilerParams(vmem_limit_bytes=40 * 1024 * 1024),
        cost_estimate=pl.CostEstimate(flops=16 * rows * depth * columns, bytes_accessed=2 * depth * columns, transcendentals=0),
        name="hidden_back",
    )(w, *parts)


def grad_kernel(width, first, count, hidden_t, *refs):
    parts = refs[:-3] if first == 0 else refs[:-4]
    out, held, sems = refs[-3:]
    slots = held.shape[0]

    def copy(index):
        slot = index % slots
        return pltpu.make_async_copy(held.at[slot], out.at[:, span(first + index, width)], sems.at[slot])

    @pl.loop(0, count)
    def _(index):
        @pl.when(index >= slots)
        def _():
            copy(index - slots).wait()

        piece = stacked([part.at[:, span(first + index, width)] for part in parts])
        held[index % slots] = dot(hidden_t[...], piece, NN).astype(BF16)
        copy(index).start()

    @pl.loop(max(0, count - slots), count)
    def _(index):
        copy(index).wait()


def grad(hidden_t, parts, calls):
    depth, rows = hidden_t.shape
    columns = parts[0].shape[1]
    width = min(1024, columns // calls)
    count = columns // width // calls
    whole = pl.BlockSpec(memory_space=pltpu.VMEM)
    anywhere = pl.BlockSpec(memory_space=pltpu.HBM)
    out = None
    for call in range(calls):
        later = call > 0
        out = pl.pallas_call(
            functools.partial(grad_kernel, width, call * count, count),
            in_specs=[whole] * (1 + len(parts)) + [anywhere] * later,
            out_specs=anywhere,
            out_shape=jax.ShapeDtypeStruct((depth, columns), BF16),
            scratch_shapes=[pltpu.VMEM((min(4, count), depth, width), BF16), pltpu.SemaphoreType.DMA((min(4, count),))],
            input_output_aliases={1 + len(parts): 0} if later else {},
            compiler_params=pltpu.CompilerParams(vmem_limit_bytes=16 * 1024 * 1024),
            cost_estimate=pl.CostEstimate(flops=16 * rows * depth * columns // calls, bytes_accessed=2 * depth * columns // calls, transcendentals=0),
            name="head_grad",
        )(hidden_t, *parts, *([out] if later else []))
    return out


def input_kernel(chosen_t, preact, mine, other, out):
    value = jnp.where(preact[...] > 0, mine[...] + other[...].astype(F32), 0.0)
    high = value.astype(BF16)
    low = (value - high.astype(F32)).astype(BF16)
    out[...] = dot(chosen_t[...], high, NN) + dot(chosen_t[...], low, NN)


def input_grad(chosen_t, preact, mine, other):
    whole = pl.BlockSpec(memory_space=pltpu.VMEM)
    return pl.pallas_call(
        input_kernel,
        in_specs=[whole] * 4,
        out_specs=whole,
        out_shape=jax.ShapeDtypeStruct((chosen_t.shape[0], preact.shape[1]), F32),
        compiler_params=pltpu.CompilerParams(vmem_limit_bytes=8 * 1024 * 1024),
        name="in_grad",
    )(chosen_t, preact, mine, other)


def swap(value, axis, bit):
    size = lax.axis_size(axis)
    return lax.ppermute(value, axis, [(i, i ^ (1 << bit)) for i in range(size)])


def gathered(value, axis):
    parts = [value]
    for bit in reversed(range(bits_of(lax.axis_size(axis)))):
        parts = parts + [swap(part, axis, bit) for part in parts]
    return parts


def local(client_ids, client_table, in_weight, in_bias, head_weight, tokens, labels, byte_table, out_table):
    head_count = lax.axis_size("head")
    group_count = lax.axis_size("client")
    columns = head_weight.shape[1]
    depth = byte_table.shape[1] * group_count
    rank = columns * head_count // (2 * depth)
    slots = client_ids.shape[0]
    place = lax.axis_index("client").astype(jnp.int32).reshape(1)
    out_parts = gathered(out_table, "client")
    byte_parts = gathered(byte_table, "client")
    keep, send, hidden_t, preact, chosen_t = forward(
        place, client_ids.reshape(1, slots), client_table, in_weight, in_bias.reshape(1, -1), head_weight, head_count, group_count
    )
    prepared = prepare(place, tokens, byte_parts, out_parts, LANES // rank)
    total = keep + swap(send, "client", 0).astype(F32)
    for bit in range(1, bits_of(group_count)):
        half = total.shape[0] // 2
        total = total[:half] + swap(total[half:].astype(BF16), "client", bit).astype(F32)
    own = total.astype(BF16).reshape(head_count, columns // LANES, LANES)
    own, prepared = lax.optimization_barrier((own, prepared))
    owned = lax.all_to_all(own, "head", split_axis=0, concat_axis=0, tiled=True)
    deltas, losses = train(rank, owned.reshape(-1, LANES), tokens, labels, prepared)
    returned = lax.all_to_all(deltas.reshape(own.shape), "head", split_axis=0, concat_axis=0, tiled=True)
    parts = gathered(returned.reshape(head_count, columns), "client")
    hidden_back = back(head_weight, parts)
    head_grad = grad(hidden_t, parts, 4)
    bits = bits_of(head_count)
    for bit in range(bits - 1):
        hidden_back = hidden_back + swap(hidden_back.astype(BF16), "head", bit).astype(F32)
    other = swap(hidden_back.astype(BF16), "head", bits - 1)
    in_grad = input_grad(chosen_t, preact, hidden_back, other)
    return head_grad, in_grad, losses[0, :1]


def solution(mesh):
    placed = (
        P(),
        P(),
        P(None, "client"),
        P("client"),
        P("client", "head"),
        P(("head", "client"), None),
        P(("head", "client"), None),
        P(None, "client"),
        P(None, "client"),
    )
    return jax.shard_map(
        local,
        mesh=mesh,
        in_specs=placed,
        out_specs=(P("client", "head"), P(None, "client"), P(("head", "client"))),
        check_vma=False,
    )
```

```python
import functools

import jax
import jax.numpy as jnp
from jax import lax
from jax.experimental import pallas as pl
from jax.experimental.pallas import tpu as pltpu
from jax.sharding import PartitionSpec as P


EPSILON = 1e-06
learn_rate = 0.1
F32 = jnp.float32
BF16 = jnp.bfloat16
LANES = 128


def dot(a, b, contract):
    return lax.dot_general(a, b, (contract, ((), ())), preferred_element_type=F32)


def split(a):
    high = a.astype(BF16)
    return high, (a - high.astype(F32)).astype(BF16)


def fine(a, b, contract):
    a_high, a_low = split(a)
    b_high, b_low = split(b)
    return dot(a_high, b_high, contract) + (dot(a_high, b_low, contract) + dot(a_low, b_high, contract))


NN = ((1,), (0,))
NT = ((1,), (1,))
TN = ((0,), (0,))


def bits_of(count):
    return count.bit_length() - 1


def offset_of(position, count):
    bits = bits_of(count)
    return sum(((position >> (bits - 1 - bit)) & 1) << bit for bit in range(bits))


def small(a, b):
    return sum(a[:, k : k + 1] * b[k : k + 1, :] for k in range(a.shape[1]))


def span(index, width):
    return pl.ds(pl.multiple_of(index * width, LANES), width)


def product_loop(width, first, hidden, w, keep, send, held, sems):
    slots = held.shape[0]
    blocks = keep.shape[1] // width
    half = keep.shape[0]

    def copy(index):
        return pltpu.make_async_copy(w.at[:, span(first + index, width)], held.at[index % slots], sems.at[index % slots])

    def start():
        @pl.loop(0, slots)
        def _(index):
            copy(index).start()

    def run():
        @pl.loop(0, blocks)
        def _(index):
            copy(index).wait()
            part = dot(hidden[...], held[index % slots], NN)
            keep[:, span(index, width)] = part[:half]
            send[:, span(index, width)] = part[half:].astype(BF16)

            @pl.when(index + slots < blocks)
            def _():
                copy(index + slots).start()

    return start, run


def first_kernel(head_count, group_count, width, place, ids, table, in_w, in_b, w, keep, send, hidden, hidden_t, preact_out, chosen_t, held, sems):
    start, run = product_loop(width, 0, hidden, w, keep, send, held, sems)
    start()
    rows = keep.shape[0] * 2
    row = lax.broadcasted_iota(jnp.int32, (rows, rows), 0)
    column = lax.broadcasted_iota(jnp.int32, (rows, rows), 1)
    position = row // head_count
    bits = bits_of(group_count)
    offset = jnp.zeros_like(position)
    for bit in range(bits):
        offset = offset + (((position >> (bits - 1 - bit)) & 1) << bit)
    slot = (row % head_count) * group_count + jnp.bitwise_xor(offset, place[0])
    picked = jnp.sum(jnp.where(column == slot, ids[...], 0), axis=1, keepdims=True)
    people = table.shape[0]
    onehot = (lax.broadcasted_iota(jnp.int32, (rows, people), 1) == picked).astype(F32).astype(BF16)
    chosen = dot(onehot, table[...], NN)
    preact = dot(chosen.astype(BF16), in_w[...], NN) + in_b[...]
    value = jnp.maximum(preact, 0.0)
    hidden[...] = value.astype(BF16)
    hidden_t[...] = value.T.astype(BF16)
    chosen_t[...] = chosen.T.astype(BF16)
    preact_out[...] = preact
    run()


def next_kernel(width, first, hidden, w, keep, send, held, sems):
    start, run = product_loop(width, first, hidden, w, keep, send, held, sems)
    start()
    run()


def forward(place, ids, table, in_w, in_b, w, head_count, group_count, calls):
    rows = ids.shape[1]
    depth, columns = w.shape
    share = columns // calls
    width = min(1024, share)
    slots = min(6, share // width)
    whole = pl.BlockSpec(memory_space=pltpu.VMEM)
    hbm = pl.BlockSpec(memory_space=pltpu.HBM)
    shapes = [((rows // 2, share), F32), ((rows // 2, share), BF16)]
    extra = [((rows, depth), BF16), ((depth, rows), BF16), ((rows, depth), F32), ((table.shape[1], rows), BF16)]
    common = dict(
        scratch_shapes=[pltpu.VMEM((slots, depth, width), BF16), pltpu.SemaphoreType.DMA((slots,))],
        compiler_params=pltpu.CompilerParams(vmem_limit_bytes=40 * 1024 * 1024),
        cost_estimate=pl.CostEstimate(flops=32 * rows * depth * share, bytes_accessed=2 * depth * share, transcendentals=0),
        name="factors",
    )
    shaped = lambda items: [jax.ShapeDtypeStruct(*shape) for shape in items]
    first = pl.pallas_call(
        functools.partial(first_kernel, head_count, group_count, width),
        in_specs=[pl.BlockSpec(memory_space=pltpu.SMEM)] + [pl.BlockSpec(value.shape) for value in (ids, table, in_w, in_b)] + [hbm],
        out_specs=[whole] * 6,
        out_shape=shaped(shapes + extra),
        **common,
    )
    keep, send, hidden, hidden_t, preact, chosen_t = first(place, ids, table, in_w, in_b, w)
    pairs = [(keep, send)]
    for call in range(1, calls):
        later = pl.pallas_call(
            functools.partial(next_kernel, width, call * (share // width)),
            in_specs=[whole, hbm],
            out_specs=[whole] * 2,
            out_shape=shaped(shapes),
            **common,
        )
        pairs.append(later(hidden, w))
    return pairs, hidden_t, preact, chosen_t


def prepare_kernel(group_count, step, place, tokens, *refs):
    near, far = refs[:group_count], refs[group_count : 3 * group_count]
    byte_full, out_full, byte_mixed, logit_gram, grams, normed_gram, inverse, squares = refs[3 * group_count :]
    vocab, width = near[0].shape
    part = vocab // 2
    turned = place[1] != 0
    depth = byte_full.shape[1]
    inner = width // step
    pair = min(2, step)
    gap = lax.broadcasted_iota(jnp.int32, (width, inner), 0) - step * lax.broadcasted_iota(jnp.int32, (width, inner), 1)
    byte_gram = jnp.zeros((vocab, vocab), F32)
    cross = jnp.zeros((vocab, vocab), F32)
    own_gram = jnp.zeros((vocab, vocab), F32)
    for position in range(group_count):
        offset = offset_of(position, group_count)
        start = jnp.bitwise_xor(place[0], offset)
        where = span(start, width)
        if offset < group_count // 2:
            out_full[:, where] = near[2 * offset][...]
            byte_full[:, where] = near[2 * offset + 1][...]
        else:
            out_low, byte_low, crossing, handed = (ref[...] for ref in far[4 * (offset - group_count // 2) :][:4])
            out_full[:part, where] = out_low
            byte_full[:part, where] = byte_low
            out_full[part:, where] = jnp.where(turned, handed, crossing)
            byte_full[part:, where] = jnp.where(turned, crossing, handed)
        out_part, byte_part = out_full[:, where], byte_full[:, where]
        byte_gram += dot(byte_part, byte_part, NT)
        cross += dot(out_part, byte_part, NT)
        own_gram += dot(out_part, out_part, NT)
    for first in range(0, step, pair):
        mixer = jnp.concatenate([jnp.where(gap == first + k, 1.0, 0.0) for k in range(pair)], axis=1).astype(BF16)
        for position in range(group_count):
            start = jnp.bitwise_xor(place[0], offset_of(position, group_count))
            mixed = dot(byte_full[:, span(start, width)], mixer, NN).astype(BF16)
            for k in range(pair):
                at = pl.multiple_of((first + k) * (depth // step) + start * inner, LANES)
                byte_mixed[:, pl.ds(at, inner)] = mixed[:, k * inner : (k + 1) * inner]
    count = tokens.shape[1]
    onehot = (lax.broadcasted_iota(jnp.int32, (vocab, count), 0) == tokens[...]).astype(F32)
    logit = fine(cross, onehot, NN)
    logit_gram[...] = logit
    half = fine(byte_gram, onehot, NN)
    total = jnp.sum(onehot * half, axis=0, keepdims=True)
    both = fine(onehot, half, TN)
    scale = lax.rsqrt(total / depth + EPSILON)
    eye = lax.broadcasted_iota(jnp.int32, (count, count), 0) == lax.broadcasted_iota(jnp.int32, (count, count), 1)
    down = jnp.sum(jnp.where(eye, scale, 0.0), axis=1, keepdims=True)
    grams[:vocab, :vocab] = own_gram
    grams[:vocab, vocab:] = logit
    grams[vocab:, :vocab] = logit.T
    grams[vocab:, vocab:] = both
    normed_gram[...] = both * scale * down
    inverse[...] = scale
    squares[...] = total


def prepare(place, tokens, near, far, step):
    group_count = len(near)
    vocab, width = near[0].shape
    count = tokens.shape[1]
    depth = width * group_count
    whole = pl.BlockSpec(memory_space=pltpu.VMEM)
    shapes = [
        ((vocab, depth), BF16),
        ((vocab, depth), BF16),
        ((vocab, depth), BF16),
        ((vocab, count), F32),
        ((vocab + count, vocab + count), F32),
        ((count, count), F32),
        ((1, count), F32),
        ((1, count), F32),
    ]
    return pl.pallas_call(
        functools.partial(prepare_kernel, group_count, step),
        in_specs=[pl.BlockSpec(memory_space=pltpu.SMEM)] + [whole] * (1 + 3 * group_count),
        out_specs=[whole] * len(shapes),
        out_shape=[jax.ShapeDtypeStruct(*shape) for shape in shapes],
        compiler_params=pltpu.CompilerParams(vmem_limit_bytes=16 * 1024 * 1024),
        cost_estimate=pl.CostEstimate(flops=2**31, bytes_accessed=2**23, transcendentals=0),
        name="prepare",
    )(place, tokens, *near, *far)


def train_kernel(
    rank,
    owned,
    tokens,
    labels,
    byte_full,
    out_full,
    byte_mixed,
    logit_gram,
    grams,
    normed_gram,
    inverse,
    squares,
    deltas,
    loss_out,
    work,
):
    vocab, depth = byte_full.shape
    count = tokens.shape[1]
    step = LANES // rank
    rows = depth * rank // LANES
    inner = depth // step
    chunks = depth // LANES
    onehot = (lax.broadcasted_iota(jnp.int32, (vocab, count), 0) == tokens[...]).astype(F32)
    label = (lax.broadcasted_iota(jnp.int32, (vocab, count), 0) == labels[...]).astype(F32)
    scale = inverse[...]
    a_t = owned[:rows, :].astype(F32).T.astype(BF16)
    table_a = jnp.zeros((rank, vocab), F32)
    for j in range(step):
        table_a += dot(a_t[j * rank : (j + 1) * rank, :], byte_mixed[:, j * inner : (j + 1) * inner], NT)
    work[...] = owned[rows:, :].astype(F32)
    b = jnp.concatenate([work[pl.ds(k, rank, stride=chunks), :] for k in range(chunks)], axis=1).astype(BF16)
    out_b = dot(b, out_full[...], NT)
    byte_b = dot(b, byte_full[...], NT)
    gram_b = dot(b, b, NT)
    low = fine(table_a, onehot, NN) * scale
    in_b = fine(byte_b, onehot, NN)
    s = 1.0 / (depth * rank) ** 0.5
    c = 4.0 / depth**0.5

    def one_step(low, both_b, gram_b):
        out_b, in_b = both_b[:, :vocab], both_b[:, vocab:]
        low_gram = small(gram_b, low)
        mean = (squares[...] + jnp.sum(low * (2.0 * s * in_b + (s * s) * low_gram), axis=0, keepdims=True)) / depth
        r = lax.rsqrt(jnp.maximum(mean, 0.0) + EPSILON)
        raw = logit_gram[...] + s * fine(out_b, low, TN)
        logits = raw * (c * r)
        top = jnp.max(logits, axis=0, keepdims=True)
        grown = jnp.exp(logits - top)
        total = jnp.sum(grown, axis=0, keepdims=True)
        loss = jnp.log(total) + top - jnp.sum(label * logits, axis=0, keepdims=True)
        error = grown / total - label
        k = (c / depth) * (r * r * r) * jnp.sum(error * raw, axis=0, keepdims=True)
        error = error * (c * r)
        d_low = s * (fine(out_b, error, NN) - k * (in_b + s * low_gram))
        kept = k * low
        on_both = rate * jnp.concatenate([-fine(low, error, NT), kept], axis=1)
        return loss, d_low, on_both, (rate * s) * fine(kept, low, NT)

    rate = learn_rate * s
    both_b = jnp.concatenate([out_b, in_b], axis=1)
    loss, d_low, on_both, more = one_step(low, both_b, gram_b)
    low_1 = low - learn_rate * fine(d_low, normed_gram[...], NN)
    both_b1 = both_b + small(more, both_b) + fine(on_both, grams[...], NN)
    gram_1 = gram_b + small(more, gram_b) + fine(on_both, both_b, NT)
    gram_b1 = gram_1 + small(gram_1, more.T) + fine(both_b1, on_both, NT)
    _, d_low1, on_both1, more1 = one_step(low_1, both_b1, gram_b1)
    total_b = more + more1 + small(more1, more)
    total_both = on_both + on_both1 + small(more1, on_both)
    total_out, total_in = total_both[:, :vocab], total_both[:, vocab:]
    on_byte = fine(total_in, onehot, NT)
    on_a = fine((-learn_rate) * scale * (d_low + d_low1), onehot, NT).astype(BF16)
    pieces = [dot(on_a, byte_mixed[:, j * inner : (j + 1) * inner], NN) for j in range(step)]
    deltas[:rows, :] = jnp.concatenate(pieces, axis=0).T.astype(BF16)
    delta_b = dot(total_b.astype(BF16), b, NN) + dot(total_out.astype(BF16), out_full[...], NN) + dot(on_byte.astype(BF16), byte_full[...], NN)
    for k in range(chunks):
        work[pl.ds(k, rank, stride=chunks), :] = delta_b[:, k * LANES : (k + 1) * LANES]
    deltas[rows:, :] = work[...].astype(BF16)
    loss_out[...] = jnp.broadcast_to(jnp.sum(loss, axis=1, keepdims=True) / count, loss_out.shape)


def train(rank, owned, tokens, labels, prepared):
    whole = pl.BlockSpec(memory_space=pltpu.VMEM)
    return pl.pallas_call(
        functools.partial(train_kernel, rank),
        in_specs=[whole] * (3 + len(prepared)),
        out_specs=[whole, whole],
        out_shape=[jax.ShapeDtypeStruct(owned.shape, BF16), jax.ShapeDtypeStruct((1, LANES), F32)],
        scratch_shapes=[pltpu.VMEM((owned.shape[0] // 2, LANES), F32)],
        compiler_params=pltpu.CompilerParams(vmem_limit_bytes=16 * 1024 * 1024),
        cost_estimate=pl.CostEstimate(flops=2**31, bytes_accessed=2**23, transcendentals=2**17),
        name="train",
    )(owned, tokens, labels, *prepared)


def stacked(parts):
    return jnp.concatenate([part[...].astype(F32) for part in parts], axis=0).astype(BF16)


def back_kernel(width, w, *refs):
    parts, out, held, sems = refs[:-3], refs[-3], refs[-2], refs[-1]
    slots = held.shape[0]
    blocks = w.shape[1] // width

    def copy(index):
        return pltpu.make_async_copy(w.at[:, span(index, width)], held.at[index % slots], sems.at[index % slots])

    @pl.loop(0, slots)
    def _(index):
        copy(index).start()

    out[...] = jnp.zeros_like(out)

    @pl.loop(0, blocks)
    def _(index):
        piece = stacked([part.at[:, span(index, width)] for part in parts])
        copy(index).wait()
        out[...] += dot(piece, held[index % slots], NT)

        @pl.when(index + slots < blocks)
        def _():
            copy(index + slots).start()


def back(w, parts):
    depth, columns = w.shape
    rows = sum(part.shape[0] for part in parts)
    width = min(1024, columns)
    slots = min(6, columns // width)
    whole = pl.BlockSpec(memory_space=pltpu.VMEM)
    return pl.pallas_call(
        functools.partial(back_kernel, width),
        in_specs=[pl.BlockSpec(memory_space=pltpu.HBM)] + [whole] * len(parts),
        out_specs=whole,
        out_shape=jax.ShapeDtypeStruct((rows, depth), F32),
        scratch_shapes=[pltpu.VMEM((slots, depth, width), BF16), pltpu.SemaphoreType.DMA((slots,))],
        compiler_params=pltpu.CompilerParams(vmem_limit_bytes=40 * 1024 * 1024),
        cost_estimate=pl.CostEstimate(flops=16 * rows * depth * columns, bytes_accessed=2 * depth * columns, transcendentals=0),
        name="hidden_back",
    )(w, *parts)


def grad_kernel(width, first, count, hidden_t, *refs):
    parts = refs[:-3] if first == 0 else refs[:-4]
    out, held, sems = refs[-3:]
    slots = held.shape[0]

    def copy(index):
        slot = index % slots
        return pltpu.make_async_copy(held.at[slot], out.at[:, span(first + index, width)], sems.at[slot])

    @pl.loop(0, count)
    def _(index):
        @pl.when(index >= slots)
        def _():
            copy(index - slots).wait()

        piece = stacked([part.at[:, span(first + index, width)] for part in parts])
        held[index % slots] = dot(hidden_t[...], piece, NN).astype(BF16)
        copy(index).start()

    @pl.loop(max(0, count - slots), count)
    def _(index):
        copy(index).wait()


def grad(hidden_t, parts, calls):
    depth, rows = hidden_t.shape
    columns = parts[0].shape[1]
    width = min(1024, columns // 4)
    blocks = columns // width
    edges = [blocks * call // calls for call in range(calls + 1)]
    whole = pl.BlockSpec(memory_space=pltpu.VMEM)
    anywhere = pl.BlockSpec(memory_space=pltpu.HBM)
    out = None
    for call in range(calls):
        later = call > 0
        count = edges[call + 1] - edges[call]
        out = pl.pallas_call(
            functools.partial(grad_kernel, width, edges[call], count),
            in_specs=[whole] * (1 + len(parts)) + [anywhere] * later,
            out_specs=anywhere,
            out_shape=jax.ShapeDtypeStruct((depth, columns), BF16),
            scratch_shapes=[pltpu.VMEM((min(4, count), depth, width), BF16), pltpu.SemaphoreType.DMA((min(4, count),))],
            input_output_aliases={1 + len(parts): 0} if later else {},
            compiler_params=pltpu.CompilerParams(vmem_limit_bytes=16 * 1024 * 1024),
            cost_estimate=pl.CostEstimate(flops=16 * rows * depth * width * count, bytes_accessed=2 * depth * width * count, transcendentals=0),
            name="head_grad",
        )(hidden_t, *parts, *([out] if later else []))
    return out


def input_kernel(chosen_t, preact, mine, other, out):
    value = jnp.where(preact[...] > 0, mine[...] + other[...].astype(F32), 0.0)
    high = value.astype(BF16)
    low = (value - high.astype(F32)).astype(BF16)
    out[...] = dot(chosen_t[...], high, NN) + dot(chosen_t[...], low, NN)


def input_grad(chosen_t, preact, mine, other):
    whole = pl.BlockSpec(memory_space=pltpu.VMEM)
    return pl.pallas_call(
        input_kernel,
        in_specs=[whole] * 4,
        out_specs=whole,
        out_shape=jax.ShapeDtypeStruct((chosen_t.shape[0], preact.shape[1]), F32),
        compiler_params=pltpu.CompilerParams(vmem_limit_bytes=8 * 1024 * 1024),
        name="in_grad",
    )(chosen_t, preact, mine, other)


def swap(value, axis, bit):
    size = lax.axis_size(axis)
    return lax.ppermute(value, axis, [(i, i ^ (1 << bit)) for i in range(size)])


def gathered(value, axis):
    parts = [value]
    for bit in reversed(range(bits_of(lax.axis_size(axis)))):
        parts = parts + [swap(part, axis, bit) for part in parts]
    return parts


def steps(client_ids, client_table, in_weight, in_bias, head_weight, tokens, labels, byte_table, out_table):
    head_count = lax.axis_size("head")
    group_count = lax.axis_size("client")
    columns = head_weight.shape[1]
    depth = byte_table.shape[1] * group_count
    rank = columns * head_count // (2 * depth)
    slots = client_ids.shape[0]
    top = bits_of(group_count) - 1
    side = lax.axis_index("head") & 1
    place = jnp.stack([lax.axis_index("client"), side]).astype(jnp.int32)
    part = out_table.shape[0] // 2
    out_low, out_high, byte_low, byte_high = out_table[:part], out_table[part:], byte_table[:part], byte_table[part:]
    crossing = swap(jnp.where(side == 0, out_high, byte_high), "client", top)
    far = [swap(out_low, "client", top), swap(byte_low, "client", top)]
    near = [out_table, byte_table]
    for bit in range(top):
        near = near + [swap(value, "client", bit) for value in near]
    pairs, hidden_t, preact, chosen_t = forward(
        place, client_ids.reshape(1, slots), client_table, in_weight, in_bias.reshape(1, -1), head_weight, head_count, group_count, 2
    )
    crossing, pairs[0] = lax.optimization_barrier((crossing, pairs[0]))
    handed = swap(crossing, "head", 0)
    far = far + [crossing, handed]
    for bit in range(top):
        far = far + [swap(value, "client", bit) for value in far]
    prepared = prepare(place, tokens, near, far, LANES // rank)
    halves = []
    for keep, send in pairs:
        total = keep + swap(send, "client", 0).astype(F32)
        for bit in range(1, top + 1):
            half = total.shape[0] // 2
            got = swap(total[half:].astype(BF16), "client", bit)
            total = total[:half] + got.astype(F32)
        halves.append(total.astype(BF16).reshape(head_count, -1, LANES))
    own = jnp.concatenate(halves, axis=1)
    own, prepared = lax.optimization_barrier((own, prepared))
    owned = lax.all_to_all(own, "head", split_axis=0, concat_axis=0, tiled=True)
    deltas, losses = train(rank, owned.reshape(-1, LANES), tokens, labels, prepared)
    returned = lax.all_to_all(deltas.reshape(own.shape), "head", split_axis=0, concat_axis=0, tiled=True)
    parts = gathered(returned.reshape(head_count, columns), "client")
    hidden_back = back(head_weight, parts)
    head_grad = grad(hidden_t, parts, 3)
    bits = bits_of(head_count)
    for bit in range(bits - 1):
        hidden_back = hidden_back + swap(hidden_back.astype(BF16), "head", bit).astype(F32)
    other = swap(hidden_back.astype(BF16), "head", bits - 1)
    in_grad = input_grad(chosen_t, preact, hidden_back, other)
    return head_grad, in_grad, losses[0, :1]


def solution(mesh):
    placed = (
        P(),
        P(),
        P(None, "client"),
        P("client"),
        P("client", "head"),
        P(("head", "client"), None),
        P(("head", "client"), None),
        P(None, "client"),
        P(None, "client"),
    )
    return jax.shard_map(
        steps,
        mesh=mesh,
        in_specs=placed,
        out_specs=(P("client", "head"), P(None, "client"), P(("head", "client"))),
        check_vma=False,
    )
```

```python
import functools

import jax
import jax.numpy as jnp
from jax import lax
from jax.experimental import pallas as pl
from jax.experimental.pallas import tpu as pltpu
from jax.sharding import PartitionSpec as P


EPSILON = 1e-06
learn_rate = 0.1
F32 = jnp.float32
BF16 = jnp.bfloat16
LANES = 128


def dot(a, b, contract):
    return lax.dot_general(a, b, (contract, ((), ())), preferred_element_type=F32)


def split(a):
    high = a.astype(BF16)
    return high, (a - high.astype(F32)).astype(BF16)


def fine(a, b, contract):
    a_high, a_low = split(a)
    b_high, b_low = split(b)
    return dot(a_high, b_high, contract) + (dot(a_high, b_low, contract) + dot(a_low, b_high, contract))


def exact(a, b, contract):
    a_high, a_low = split(a)
    picked = b.astype(BF16)
    return dot(a_high, picked, contract) + dot(a_low, picked, contract)


NN = ((1,), (0,))
NT = ((1,), (1,))
TN = ((0,), (0,))


def bits_of(count):
    return count.bit_length() - 1


def small(a, b):
    return sum(a[:, k : k + 1] * b[k : k + 1, :] for k in range(a.shape[1]))


def span(index, width):
    return pl.ds(pl.multiple_of(index * width, LANES), width)


def product_loop(width, first, hidden, w, keep, send, held, sems):
    slots = held.shape[0]
    blocks = keep.shape[1] // width
    half = keep.shape[0]

    def copy(index):
        return pltpu.make_async_copy(w.at[:, span(first + index, width)], held.at[index % slots], sems.at[index % slots])

    def start():
        @pl.loop(0, slots)
        def _(index):
            copy(index).start()

    def run():
        @pl.loop(0, blocks)
        def _(index):
            copy(index).wait()
            part = dot(hidden[...], held[index % slots], NN)
            keep[:, span(index, width)] = part[:half]
            send[:, span(index, width)] = part[half:].astype(BF16)

            @pl.when(index + slots < blocks)
            def _():
                copy(index + slots).start()

    return start, run


def first_kernel(head_count, group_count, width, people, place, row_values, matrices, w, keep, send, hidden, hidden_t, preact_out, chosen_t, held, sems):
    start, run = product_loop(width, 0, hidden, w, keep, send, held, sems)
    start()
    rows = keep.shape[0] * 2
    embed = chosen_t.shape[0]
    depth = hidden.shape[1]
    row = lax.broadcasted_iota(jnp.int32, (rows, rows), 0)
    column = lax.broadcasted_iota(jnp.int32, (rows, rows), 1)
    position = row // head_count
    bits = bits_of(group_count)
    offset = jnp.zeros_like(position)
    for bit in range(bits):
        offset = offset + (((position >> (bits - 1 - bit)) & 1) << bit)
    slot = (row % head_count) * group_count + jnp.bitwise_xor(offset, place[0])
    picked = jnp.sum(jnp.where(column == slot, row_values[:, depth:], 0.0), axis=1, keepdims=True).astype(jnp.int32)
    onehot = (lax.broadcasted_iota(jnp.int32, (rows, people), 1) == picked).astype(F32).astype(BF16)
    chosen = dot(onehot, matrices[:people, depth:], NN)
    preact = dot(chosen.astype(BF16), matrices[:embed, :depth], NN) + row_values[:, :depth]
    value = jnp.maximum(preact, 0.0)
    hidden[...] = value.astype(BF16)
    hidden_t[...] = value.T.astype(BF16)
    chosen_t[...] = chosen.T.astype(BF16)
    preact_out[...] = preact
    run()


def next_kernel(width, first, hidden, w, keep, send, held, sems):
    start, run = product_loop(width, first, hidden, w, keep, send, held, sems)
    start()
    run()


def forward(place, ids, table, in_w, in_b, w, head_count, group_count, calls):
    rows = ids.shape[0]
    people, embed = table.shape
    row_values = jnp.concatenate([in_b, ids.astype(F32)]).reshape(1, -1)
    tall = max(people, embed)
    matrices = jnp.concatenate([jnp.pad(value, ((0, tall - value.shape[0]), (0, 0))) for value in (in_w, table)], axis=1)
    depth, columns = w.shape
    share = columns // calls
    width = min(1024, share)
    slots = min(6, share // width)
    whole = pl.BlockSpec(memory_space=pltpu.VMEM)
    hbm = pl.BlockSpec(memory_space=pltpu.HBM)
    shapes = [((rows // 2, share), F32), ((rows // 2, share), BF16)]
    extra = [((rows, depth), BF16), ((depth, rows), BF16), ((rows, depth), F32), ((embed, rows), BF16)]
    common = dict(
        scratch_shapes=[pltpu.VMEM((slots, depth, width), BF16), pltpu.SemaphoreType.DMA((slots,))],
        compiler_params=pltpu.CompilerParams(vmem_limit_bytes=40 * 1024 * 1024),
        cost_estimate=pl.CostEstimate(flops=32 * rows * depth * share, bytes_accessed=2 * depth * share, transcendentals=0),
        name="factors",
    )
    shaped = lambda items: [jax.ShapeDtypeStruct(*shape) for shape in items]
    first = pl.pallas_call(
        functools.partial(first_kernel, head_count, group_count, width, people),
        in_specs=[pl.BlockSpec(memory_space=pltpu.SMEM)] + [whole] * 2 + [hbm],
        out_specs=[whole] * 6,
        out_shape=shaped(shapes + extra),
        **common,
    )
    keep, send, hidden, hidden_t, preact, chosen_t = first(place, row_values, matrices, w)
    pairs = [(keep, send)]
    for call in range(1, calls):
        later = pl.pallas_call(
            functools.partial(next_kernel, width, call * (share // width)),
            in_specs=[whole, hbm],
            out_specs=[whole] * 2,
            out_shape=shaped(shapes),
            **common,
        )
        pairs.append(later(hidden, w))
    return pairs, hidden_t, preact, chosen_t


def products(out_part, byte_part):
    return dot(byte_part, byte_part, NT), dot(out_part, byte_part, NT), dot(out_part, out_part, NT)


def mixers(width, step):
    inner = width // step
    gap = lax.broadcasted_iota(jnp.int32, (width, inner), 0) - step * lax.broadcasted_iota(jnp.int32, (width, inner), 1)
    pair = min(2, step)
    return [
        (first, jnp.concatenate([jnp.where(gap == first + k, 1.0, 0.0) for k in range(pair)], axis=1).astype(BF16))
        for first in range(0, step, pair)
    ]


def near_kernel(step, *refs):
    near, (byte_gram, cross, own_gram, mixed) = refs[:-4], refs[-4:]
    width = near[0].shape[1]
    inner = width // step
    sums = [jnp.zeros(ref.shape, F32) for ref in (byte_gram, cross, own_gram)]
    for index in range(len(near) // 2):
        out_part, byte_part = near[2 * index][...], near[2 * index + 1][...]
        sums = [total + value for total, value in zip(sums, products(out_part, byte_part))]
        for first, mixer in mixers(width, step):
            at = index * width + first * inner
            mixed[:, at : at + mixer.shape[1]] = dot(byte_part, mixer, NN).astype(BF16)
    byte_gram[...], cross[...], own_gram[...] = sums


def prepare_kernel(group_count, step, place, tokens, *refs):
    half = group_count // 2
    near, far, known = refs[:group_count], refs[group_count : group_count + 3 * half], refs[group_count + 3 * half :][:4]
    byte_full, out_full, byte_mixed, logit_gram, grams, normed_gram, inverse, squares = refs[group_count + 3 * half + 4 :]
    vocab, width = near[0].shape
    part = vocab // 2
    turned = place[1] != 0
    depth = byte_full.shape[1]
    inner = width // step
    byte_gram, cross, own_gram = (ref[...] for ref in known[:3])
    for offset in range(group_count):
        start = jnp.bitwise_xor(place[0], offset)
        where = span(start, width)

        def mixed_at(j):
            return pl.ds(pl.multiple_of(j * (depth // step) + start * inner, LANES), inner)

        if offset < half:
            out_full[:, where] = near[2 * offset][...]
            byte_full[:, where] = near[2 * offset + 1][...]
            for j in range(step):
                at = offset * width + j * inner
                byte_mixed[:, mixed_at(j)] = known[3][:, at : at + inner]
            continue
        lows, crossing, handed = (ref[...] for ref in far[3 * (offset - half) :][:3])
        out_full[:part, where] = lows[:part]
        byte_full[:part, where] = lows[part:]
        out_full[part:, where] = jnp.where(turned, handed, crossing)
        byte_full[part:, where] = jnp.where(turned, crossing, handed)
        out_part, byte_part = out_full[:, where], byte_full[:, where]
        values = products(out_part, byte_part)
        byte_gram, cross, own_gram = byte_gram + values[0], cross + values[1], own_gram + values[2]
        for first, mixer in mixers(width, step):
            mixed = dot(byte_part, mixer, NN).astype(BF16)
            for k in range(mixer.shape[1] // inner):
                byte_mixed[:, mixed_at(first + k)] = mixed[:, k * inner : (k + 1) * inner]
    count = tokens.shape[1]
    onehot = (lax.broadcasted_iota(jnp.int32, (vocab, count), 0) == tokens[...]).astype(F32)
    logit = exact(cross, onehot, NN)
    logit_gram[...] = logit
    picked = exact(byte_gram, onehot, NN)
    total = jnp.sum(onehot * picked, axis=0, keepdims=True)
    picked_high, picked_low = split(picked)
    both = dot(onehot.astype(BF16), picked_high, TN) + dot(onehot.astype(BF16), picked_low, TN)
    scale = lax.rsqrt(total / depth + EPSILON)
    eye = lax.broadcasted_iota(jnp.int32, (count, count), 0) == lax.broadcasted_iota(jnp.int32, (count, count), 1)
    down = jnp.sum(jnp.where(eye, scale, 0.0), axis=1, keepdims=True)
    grams[:vocab, :vocab] = own_gram
    grams[:vocab, vocab:] = logit
    grams[vocab:, :vocab] = logit.T
    grams[vocab:, vocab:] = both
    normed_gram[...] = both * scale * down
    inverse[...] = scale
    squares[...] = total


def prepare(place, tokens, near, far, step):
    group_count = len(near)
    vocab, width = near[0].shape
    count = tokens.shape[1]
    depth = width * group_count
    whole = pl.BlockSpec(memory_space=pltpu.VMEM)
    shaped = lambda shapes: [jax.ShapeDtypeStruct(*shape) for shape in shapes]
    known_shapes = [((vocab, vocab), F32)] * 3 + [((vocab, depth // 2), BF16)]
    known = pl.pallas_call(
        functools.partial(near_kernel, step),
        in_specs=[whole] * len(near),
        out_specs=[whole] * 4,
        out_shape=shaped(known_shapes),
        compiler_params=pltpu.CompilerParams(vmem_limit_bytes=16 * 1024 * 1024),
        cost_estimate=pl.CostEstimate(flops=2**30, bytes_accessed=2**22, transcendentals=0),
        name="prepare_near",
    )(*near)
    shapes = [
        ((vocab, depth), BF16),
        ((vocab, depth), BF16),
        ((vocab, depth), BF16),
        ((vocab, count), F32),
        ((vocab + count, vocab + count), F32),
        ((count, count), F32),
        ((1, count), F32),
        ((1, count), F32),
    ]
    return pl.pallas_call(
        functools.partial(prepare_kernel, group_count, step),
        in_specs=[pl.BlockSpec(memory_space=pltpu.SMEM)] + [whole] * (5 + len(near) + len(far)),
        out_specs=[whole] * len(shapes),
        out_shape=shaped(shapes),
        compiler_params=pltpu.CompilerParams(vmem_limit_bytes=16 * 1024 * 1024),
        cost_estimate=pl.CostEstimate(flops=2**30, bytes_accessed=2**23, transcendentals=0),
        name="prepare",
    )(place, tokens, *near, *far, *known)


def train_kernel(
    rank,
    owned,
    tokens,
    labels,
    byte_full,
    out_full,
    byte_mixed,
    logit_gram,
    grams,
    normed_gram,
    inverse,
    squares,
    deltas,
    loss_out,
    work,
):
    vocab, depth = byte_full.shape
    count = tokens.shape[1]
    step = LANES // rank
    rows = depth * rank // LANES
    inner = depth // step
    chunks = depth // LANES
    onehot = (lax.broadcasted_iota(jnp.int32, (vocab, count), 0) == tokens[...]).astype(F32)
    label = (lax.broadcasted_iota(jnp.int32, (vocab, count), 0) == labels[...]).astype(F32)
    scale = inverse[...]
    a_t = owned[:rows, :].astype(F32).T.astype(BF16)
    table_a = jnp.zeros((rank, vocab), F32)
    for j in range(step):
        table_a += dot(a_t[j * rank : (j + 1) * rank, :], byte_mixed[:, j * inner : (j + 1) * inner], NT)
    work[...] = owned[rows:, :].astype(F32)
    b = jnp.concatenate([work[pl.ds(k, rank, stride=chunks), :] for k in range(chunks)], axis=1).astype(BF16)
    out_b = dot(b, out_full[...], NT)
    byte_b = dot(b, byte_full[...], NT)
    gram_b = dot(b, b, NT)
    low = exact(table_a, onehot, NN) * scale
    in_b = exact(byte_b, onehot, NN)
    s = 1.0 / (depth * rank) ** 0.5
    c = 4.0 / depth**0.5

    def one_step(low, both_b, gram_b):
        out_b, in_b = both_b[:, :vocab], both_b[:, vocab:]
        low_gram = small(gram_b, low)
        mean = (squares[...] + jnp.sum(low * (2.0 * s * in_b + (s * s) * low_gram), axis=0, keepdims=True)) / depth
        r = lax.rsqrt(jnp.maximum(mean, 0.0) + EPSILON)
        raw = logit_gram[...] + s * fine(out_b, low, TN)
        logits = raw * (c * r)
        top = jnp.max(logits, axis=0, keepdims=True)
        grown = jnp.exp(logits - top)
        total = jnp.sum(grown, axis=0, keepdims=True)
        loss = jnp.log(total) + top - jnp.sum(label * logits, axis=0, keepdims=True)
        error = grown / total - label
        k = (c / depth) * (r * r * r) * jnp.sum(error * raw, axis=0, keepdims=True)
        error = error * (c * r)
        d_low = s * (fine(out_b, error, NN) - k * (in_b + s * low_gram))
        kept = k * low
        on_both = rate * jnp.concatenate([-fine(low, error, NT), kept], axis=1)
        return loss, d_low, on_both, (rate * s) * fine(kept, low, NT)

    rate = learn_rate * s
    both_b = jnp.concatenate([out_b, in_b], axis=1)
    loss, d_low, on_both, more = one_step(low, both_b, gram_b)
    low_1 = low - learn_rate * fine(d_low, normed_gram[...], NN)
    both_b1 = both_b + small(more, both_b) + fine(on_both, grams[...], NN)
    gram_1 = gram_b + small(more, gram_b) + fine(on_both, both_b, NT)
    gram_b1 = gram_1 + small(gram_1, more.T) + fine(both_b1, on_both, NT)
    _, d_low1, on_both1, more1 = one_step(low_1, both_b1, gram_b1)
    total_b = more + more1 + small(more1, more)
    total_both = on_both + on_both1 + small(more1, on_both)
    total_out, total_in = total_both[:, :vocab], total_both[:, vocab:]
    on_byte = exact(total_in, onehot, NT)
    on_a = exact((-learn_rate) * scale * (d_low + d_low1), onehot, NT).astype(BF16)
    pieces = [dot(on_a, byte_mixed[:, j * inner : (j + 1) * inner], NN) for j in range(step)]
    deltas[:rows, :] = jnp.concatenate(pieces, axis=0).T.astype(BF16)
    delta_b = dot(total_b.astype(BF16), b, NN) + dot(total_out.astype(BF16), out_full[...], NN) + dot(on_byte.astype(BF16), byte_full[...], NN)
    for k in range(chunks):
        work[pl.ds(k, rank, stride=chunks), :] = delta_b[:, k * LANES : (k + 1) * LANES]
    deltas[rows:, :] = work[...].astype(BF16)
    loss_out[...] = jnp.broadcast_to(jnp.sum(loss, axis=1, keepdims=True) / count, loss_out.shape)


def train(rank, owned, tokens, labels, prepared):
    whole = pl.BlockSpec(memory_space=pltpu.VMEM)
    return pl.pallas_call(
        functools.partial(train_kernel, rank),
        in_specs=[whole] * (3 + len(prepared)),
        out_specs=[whole, whole],
        out_shape=[jax.ShapeDtypeStruct(owned.shape, BF16), jax.ShapeDtypeStruct((1, LANES), F32)],
        scratch_shapes=[pltpu.VMEM((owned.shape[0] // 2, LANES), F32)],
        compiler_params=pltpu.CompilerParams(vmem_limit_bytes=16 * 1024 * 1024),
        cost_estimate=pl.CostEstimate(flops=2**31, bytes_accessed=2**23, transcendentals=2**17),
        name="train",
    )(owned, tokens, labels, *prepared)


def stacked(parts):
    return jnp.concatenate([part[...].astype(F32) for part in parts], axis=0).astype(BF16)


def back_kernel(width, w, *refs):
    parts, out, held, sems = refs[:-3], refs[-3], refs[-2], refs[-1]
    slots = held.shape[0]
    blocks = w.shape[1] // width

    def copy(index):
        return pltpu.make_async_copy(w.at[:, span(index, width)], held.at[index % slots], sems.at[index % slots])

    @pl.loop(0, slots)
    def _(index):
        copy(index).start()

    out[...] = jnp.zeros_like(out)

    @pl.loop(0, blocks)
    def _(index):
        piece = stacked([part.at[:, span(index, width)] for part in parts])
        copy(index).wait()
        out[...] += dot(piece, held[index % slots], NT)

        @pl.when(index + slots < blocks)
        def _():
            copy(index + slots).start()


def back(w, parts):
    depth, columns = w.shape
    rows = sum(part.shape[0] for part in parts)
    width = min(2048, columns)
    slots = min(4, columns // width)
    whole = pl.BlockSpec(memory_space=pltpu.VMEM)
    return pl.pallas_call(
        functools.partial(back_kernel, width),
        in_specs=[pl.BlockSpec(memory_space=pltpu.HBM)] + [whole] * len(parts),
        out_specs=whole,
        out_shape=jax.ShapeDtypeStruct((rows, depth), F32),
        scratch_shapes=[pltpu.VMEM((slots, depth, width), BF16), pltpu.SemaphoreType.DMA((slots,))],
        compiler_params=pltpu.CompilerParams(vmem_limit_bytes=40 * 1024 * 1024),
        cost_estimate=pl.CostEstimate(flops=16 * rows * depth * columns, bytes_accessed=2 * depth * columns, transcendentals=0),
        name="hidden_back",
    )(w, *parts)


def grad_kernel(width, first, count, hidden_t, *refs):
    parts = refs[:-3] if first == 0 else refs[:-4]
    out, held, sems = refs[-3:]
    slots = held.shape[0]

    def copy(index):
        slot = index % slots
        return pltpu.make_async_copy(held.at[slot], out.at[:, span(first + index, width)], sems.at[slot])

    @pl.loop(0, count)
    def _(index):
        @pl.when(index >= slots)
        def _():
            copy(index - slots).wait()

        piece = stacked([part.at[:, span(first + index, width)] for part in parts])
        held[index % slots] = dot(hidden_t[...], piece, NN).astype(BF16)
        copy(index).start()

    @pl.loop(max(0, count - slots), count)
    def _(index):
        copy(index).wait()


def grad(hidden_t, parts, calls):
    depth, rows = hidden_t.shape
    columns = parts[0].shape[1]
    width = min(1024, columns // 4)
    blocks = columns // width
    edges = [blocks * call // calls for call in range(calls + 1)]
    whole = pl.BlockSpec(memory_space=pltpu.VMEM)
    anywhere = pl.BlockSpec(memory_space=pltpu.HBM)
    out = None
    for call in range(calls):
        later = call > 0
        count = edges[call + 1] - edges[call]
        out = pl.pallas_call(
            functools.partial(grad_kernel, width, edges[call], count),
            in_specs=[whole] * (1 + len(parts)) + [anywhere] * later,
            out_specs=anywhere,
            out_shape=jax.ShapeDtypeStruct((depth, columns), BF16),
            scratch_shapes=[pltpu.VMEM((min(4, count), depth, width), BF16), pltpu.SemaphoreType.DMA((min(4, count),))],
            input_output_aliases={1 + len(parts): 0} if later else {},
            compiler_params=pltpu.CompilerParams(vmem_limit_bytes=16 * 1024 * 1024),
            cost_estimate=pl.CostEstimate(flops=16 * rows * depth * width * count, bytes_accessed=2 * depth * width * count, transcendentals=0),
            name="head_grad",
        )(hidden_t, *parts, *([out] if later else []))
    return out


def input_kernel(chosen_t, preact, mine, other, out):
    value = jnp.where(preact[...] > 0, mine[...] + other[...].astype(F32), 0.0)
    high = value.astype(BF16)
    low = (value - high.astype(F32)).astype(BF16)
    out[...] = dot(chosen_t[...], high, NN) + dot(chosen_t[...], low, NN)


def input_grad(chosen_t, preact, mine, other):
    whole = pl.BlockSpec(memory_space=pltpu.VMEM)
    return pl.pallas_call(
        input_kernel,
        in_specs=[whole] * 4,
        out_specs=whole,
        out_shape=jax.ShapeDtypeStruct((chosen_t.shape[0], preact.shape[1]), F32),
        compiler_params=pltpu.CompilerParams(vmem_limit_bytes=8 * 1024 * 1024),
        name="in_grad",
    )(chosen_t, preact, mine, other)


def swap(value, axis, bit):
    size = lax.axis_size(axis)
    return lax.ppermute(value, axis, [(i, i ^ (1 << bit)) for i in range(size)])


def gathered(value, axis):
    parts = [value]
    for bit in reversed(range(bits_of(lax.axis_size(axis)))):
        parts = parts + [swap(part, axis, bit) for part in parts]
    return parts


def steps(client_ids, client_table, in_weight, in_bias, head_weight, tokens, labels, byte_table, out_table):
    head_count = lax.axis_size("head")
    group_count = lax.axis_size("client")
    columns = head_weight.shape[1]
    depth = byte_table.shape[1] * group_count
    rank = columns * head_count // (2 * depth)
    top = bits_of(group_count) - 1
    side = lax.axis_index("head") & 1
    place = jnp.stack([lax.axis_index("client"), side]).astype(jnp.int32)
    part = out_table.shape[0] // 2
    out_low, out_high, byte_low, byte_high = out_table[:part], out_table[part:], byte_table[:part], byte_table[part:]
    crossing = swap(jnp.where(side == 0, out_high, byte_high), "client", top)
    far = [swap(jnp.concatenate([out_low, byte_low]), "client", top)]
    near = [out_table, byte_table]
    for bit in range(top):
        near = near + [swap(value, "client", bit) for value in near]
    pairs, hidden_t, preact, chosen_t = forward(
        place, client_ids, client_table, in_weight, in_bias, head_weight, head_count, group_count, 2
    )
    crossing, pairs[0] = lax.optimization_barrier((crossing, pairs[0]))
    handed = swap(crossing, "head", 0)
    far, late = far + [crossing], [handed]
    for bit in range(top):
        far = far + [swap(value, "client", bit) for value in far]
        late = late + [swap(value, "client", bit) for value in late]
    far = [value for at in range(1 << top) for value in (*far[2 * at : 2 * at + 2], late[at])]
    prepared = prepare(place, tokens, near, far, LANES // rank)
    halves = []
    for keep, send in pairs:
        got = swap(send, "client", 0)
        total = keep + got.astype(F32)
        for bit in range(1, top + 1):
            half = total.shape[0] // 2
            got = swap(total[half:].astype(BF16), "client", bit)
            total = total[:half] + got.astype(F32)
        halves.append(total.astype(BF16).reshape(head_count, -1, LANES))
    own = jnp.concatenate(halves, axis=1)
    own, prepared = lax.optimization_barrier((own, prepared))
    owned = lax.all_to_all(own, "head", split_axis=0, concat_axis=0, tiled=True)
    deltas, losses = train(rank, owned.reshape(-1, LANES), tokens, labels, prepared)
    returned = lax.all_to_all(deltas.reshape(own.shape), "head", split_axis=0, concat_axis=0, tiled=True)
    parts = gathered(returned.reshape(head_count, columns), "client")
    hidden_back = back(head_weight, parts)
    head_grad = grad(hidden_t, parts, 3)
    bits = bits_of(head_count)
    for bit in range(bits - 1):
        hidden_back = hidden_back + swap(hidden_back.astype(BF16), "head", bit).astype(F32)
    other = swap(hidden_back.astype(BF16), "head", bits - 1)
    in_grad = input_grad(chosen_t, preact, hidden_back, other)
    return head_grad, in_grad, losses[0, :1]


def solution(mesh):
    placed = (
        P(),
        P(),
        P(None, "client"),
        P("client"),
        P("client", "head"),
        P(("head", "client"), None),
        P(("head", "client"), None),
        P(None, "client"),
        P(None, "client"),
    )
    return jax.shard_map(
        steps,
        mesh=mesh,
        in_specs=placed,
        out_specs=(P("client", "head"), P(None, "client"), P(("head", "client"))),
        check_vma=False,
    )
```

```python
import functools

import jax
import jax.numpy as jnp
from jax import lax
from jax.experimental import pallas as pl
from jax.experimental.pallas import tpu as pltpu
from jax.sharding import PartitionSpec as P


EPSILON = 1e-06
learn_rate = 0.1
F32 = jnp.float32
BF16 = jnp.bfloat16
LANES = 128


def dot(a, b, contract):
    return lax.dot_general(a, b, (contract, ((), ())), preferred_element_type=F32)


def split(a):
    high = a.astype(BF16)
    return high, (a - high.astype(F32)).astype(BF16)


def fine(a, b, contract):
    a_high, a_low = split(a)
    b_high, b_low = split(b)
    return dot(a_high, b_high, contract) + (dot(a_high, b_low, contract) + dot(a_low, b_high, contract))


def exact(a, b, contract):
    a_high, a_low = split(a)
    picked = b.astype(BF16)
    return dot(a_high, picked, contract) + dot(a_low, picked, contract)


NN = ((1,), (0,))
NT = ((1,), (1,))
TN = ((0,), (0,))


def bits_of(count):
    return count.bit_length() - 1


def small(a, b):
    return sum(a[:, k : k + 1] * b[k : k + 1, :] for k in range(a.shape[1]))


def span(index, width):
    return pl.ds(pl.multiple_of(index * width, LANES), width)


def product_loop(width, first, hidden, w, keep, send, held, sems):
    slots = held.shape[0]
    blocks = keep.shape[1] // width
    half = keep.shape[0]

    def copy(index):
        return pltpu.make_async_copy(w.at[:, span(first + index, width)], held.at[index % slots], sems.at[index % slots])

    def start():
        @pl.loop(0, slots)
        def _(index):
            copy(index).start()

    def run():
        @pl.loop(0, blocks)
        def _(index):
            copy(index).wait()
            part = dot(hidden[...], held[index % slots], NN)
            keep[:, span(index, width)] = part[:half]
            send[:, span(index, width)] = part[half:].astype(BF16)

            @pl.when(index + slots < blocks)
            def _():
                copy(index + slots).start()

    return start, run


def first_kernel(head_count, group_count, width, people, place, row_values, matrices, w, keep, send, hidden, hidden_t, preact_out, chosen_t, held, sems):
    start, run = product_loop(width, 0, hidden, w, keep, send, held, sems)
    start()
    rows = keep.shape[0] * 2
    embed = chosen_t.shape[0]
    depth = hidden.shape[1]
    row = lax.broadcasted_iota(jnp.int32, (rows, rows), 0)
    column = lax.broadcasted_iota(jnp.int32, (rows, rows), 1)
    position = row // head_count
    bits = bits_of(group_count)
    offset = jnp.zeros_like(position)
    for bit in range(bits):
        offset = offset + (((position >> (bits - 1 - bit)) & 1) << bit)
    slot = (row % head_count) * group_count + jnp.bitwise_xor(offset, place[0])
    picked = jnp.sum(jnp.where(column == slot, row_values[:, depth:], 0.0), axis=1, keepdims=True).astype(jnp.int32)
    onehot = (lax.broadcasted_iota(jnp.int32, (rows, people), 1) == picked).astype(F32).astype(BF16)
    chosen = dot(onehot, matrices[:people, depth:], NN)
    preact = dot(chosen.astype(BF16), matrices[:embed, :depth], NN) + row_values[:, :depth]
    value = jnp.maximum(preact, 0.0)
    hidden[...] = value.astype(BF16)
    hidden_t[...] = value.T.astype(BF16)
    chosen_t[...] = chosen.T.astype(BF16)
    preact_out[...] = preact
    run()


def next_kernel(width, first, hidden, w, keep, send, held, sems):
    start, run = product_loop(width, first, hidden, w, keep, send, held, sems)
    start()
    run()


def forward(place, ids, table, in_w, in_b, w, head_count, group_count, calls):
    rows = ids.shape[0]
    people, embed = table.shape
    row_values = jnp.concatenate([in_b, ids.astype(F32)]).reshape(1, -1)
    tall = max(people, embed)
    matrices = jnp.concatenate([jnp.pad(value, ((0, tall - value.shape[0]), (0, 0))) for value in (in_w, table)], axis=1)
    depth, columns = w.shape
    share = columns // calls
    width = min(1024, share)
    slots = min(6, share // width)
    whole = pl.BlockSpec(memory_space=pltpu.VMEM)
    hbm = pl.BlockSpec(memory_space=pltpu.HBM)
    shapes = [((rows // 2, share), F32), ((rows // 2, share), BF16)]
    extra = [((rows, depth), BF16), ((depth, rows), BF16), ((rows, depth), F32), ((embed, rows), BF16)]
    common = dict(
        scratch_shapes=[pltpu.VMEM((slots, depth, width), BF16), pltpu.SemaphoreType.DMA((slots,))],
        compiler_params=pltpu.CompilerParams(vmem_limit_bytes=40 * 1024 * 1024),
        cost_estimate=pl.CostEstimate(flops=32 * rows * depth * share, bytes_accessed=2 * depth * share, transcendentals=0),
        name="factors",
    )
    shaped = lambda items: [jax.ShapeDtypeStruct(*shape) for shape in items]
    first = pl.pallas_call(
        functools.partial(first_kernel, head_count, group_count, width, people),
        in_specs=[pl.BlockSpec(memory_space=pltpu.SMEM)] + [whole] * 2 + [hbm],
        out_specs=[whole] * 6,
        out_shape=shaped(shapes + extra),
        **common,
    )
    keep, send, hidden, hidden_t, preact, chosen_t = first(place, row_values, matrices, w)
    pairs = [(keep, send)]
    for call in range(1, calls):
        later = pl.pallas_call(
            functools.partial(next_kernel, width, call * (share // width)),
            in_specs=[whole, hbm],
            out_specs=[whole] * 2,
            out_shape=shaped(shapes),
            **common,
        )
        pairs.append(later(hidden, w))
    return pairs, hidden_t, preact, chosen_t


def products(out_part, byte_part):
    return dot(byte_part, byte_part, NT), dot(out_part, byte_part, NT), dot(out_part, out_part, NT)


def mixers(width, step):
    inner = width // step
    gap = lax.broadcasted_iota(jnp.int32, (width, inner), 0) - step * lax.broadcasted_iota(jnp.int32, (width, inner), 1)
    pair = min(2, step)
    return [
        (first, jnp.concatenate([jnp.where(gap == first + k, 1.0, 0.0) for k in range(pair)], axis=1).astype(BF16))
        for first in range(0, step, pair)
    ]


def near_kernel(step, *refs):
    near, (byte_gram, cross, own_gram, mixed) = refs[:-4], refs[-4:]
    width = near[0].shape[1]
    inner = width // step
    sums = [jnp.zeros(ref.shape, F32) for ref in (byte_gram, cross, own_gram)]
    for index in range(len(near) // 2):
        out_part, byte_part = near[2 * index][...], near[2 * index + 1][...]
        sums = [total + value for total, value in zip(sums, products(out_part, byte_part))]
        for first, mixer in mixers(width, step):
            at = index * width + first * inner
            mixed[:, at : at + mixer.shape[1]] = dot(byte_part, mixer, NN).astype(BF16)
    byte_gram[...], cross[...], own_gram[...] = sums


def prepare_kernel(group_count, step, place, tokens, *refs):
    half = group_count // 2
    near, far, known = refs[:group_count], refs[group_count : group_count + 3 * half], refs[group_count + 3 * half :][:4]
    byte_full, out_full, byte_mixed, logit_gram, grams, normed_gram, inverse, squares = refs[group_count + 3 * half + 4 :]
    vocab, width = near[0].shape
    part = vocab // 2
    turned = place[1] != 0
    depth = byte_full.shape[1]
    inner = width // step
    byte_gram, cross, own_gram = (ref[...] for ref in known[:3])
    for offset in range(group_count):
        start = jnp.bitwise_xor(place[0], offset)
        where = span(start, width)

        def mixed_at(j):
            return pl.ds(pl.multiple_of(j * (depth // step) + start * inner, LANES), inner)

        if offset < half:
            out_full[:, where] = near[2 * offset][...]
            byte_full[:, where] = near[2 * offset + 1][...]
            for j in range(step):
                at = offset * width + j * inner
                byte_mixed[:, mixed_at(j)] = known[3][:, at : at + inner]
            continue
        lows, crossing, handed = (ref[...] for ref in far[3 * (offset - half) :][:3])
        out_full[:part, where] = lows[:part]
        byte_full[:part, where] = lows[part:]
        out_full[part:, where] = jnp.where(turned, handed, crossing)
        byte_full[part:, where] = jnp.where(turned, crossing, handed)
        out_part, byte_part = out_full[:, where], byte_full[:, where]
        values = products(out_part, byte_part)
        byte_gram, cross, own_gram = byte_gram + values[0], cross + values[1], own_gram + values[2]
        for first, mixer in mixers(width, step):
            mixed = dot(byte_part, mixer, NN).astype(BF16)
            for k in range(mixer.shape[1] // inner):
                byte_mixed[:, mixed_at(first + k)] = mixed[:, k * inner : (k + 1) * inner]
    count = tokens.shape[1]
    onehot = (lax.broadcasted_iota(jnp.int32, (vocab, count), 0) == tokens[...]).astype(F32)
    logit = exact(cross, onehot, NN)
    logit_gram[...] = logit
    picked = exact(byte_gram, onehot, NN)
    total = jnp.sum(onehot * picked, axis=0, keepdims=True)
    picked_high, picked_low = split(picked)
    both = dot(onehot.astype(BF16), picked_high, TN) + dot(onehot.astype(BF16), picked_low, TN)
    scale = lax.rsqrt(total / depth + EPSILON)
    eye = lax.broadcasted_iota(jnp.int32, (count, count), 0) == lax.broadcasted_iota(jnp.int32, (count, count), 1)
    down = jnp.sum(jnp.where(eye, scale, 0.0), axis=1, keepdims=True)
    grams[:vocab, :vocab] = own_gram
    grams[:vocab, vocab:] = logit
    grams[vocab:, :vocab] = logit.T
    grams[vocab:, vocab:] = both
    normed_gram[...] = both * scale * down
    inverse[...] = scale
    squares[...] = total


def prepare(place, tokens, near, far, step):
    group_count = len(near)
    vocab, width = near[0].shape
    count = tokens.shape[1]
    depth = width * group_count
    whole = pl.BlockSpec(memory_space=pltpu.VMEM)
    shaped = lambda shapes: [jax.ShapeDtypeStruct(*shape) for shape in shapes]
    known_shapes = [((vocab, vocab), F32)] * 3 + [((vocab, depth // 2), BF16)]
    known = pl.pallas_call(
        functools.partial(near_kernel, step),
        in_specs=[whole] * len(near),
        out_specs=[whole] * 4,
        out_shape=shaped(known_shapes),
        compiler_params=pltpu.CompilerParams(vmem_limit_bytes=16 * 1024 * 1024),
        cost_estimate=pl.CostEstimate(flops=2**30, bytes_accessed=2**22, transcendentals=0),
        name="prepare_near",
    )(*near)
    shapes = [
        ((vocab, depth), BF16),
        ((vocab, depth), BF16),
        ((vocab, depth), BF16),
        ((vocab, count), F32),
        ((vocab + count, vocab + count), F32),
        ((count, count), F32),
        ((1, count), F32),
        ((1, count), F32),
    ]
    return pl.pallas_call(
        functools.partial(prepare_kernel, group_count, step),
        in_specs=[pl.BlockSpec(memory_space=pltpu.SMEM)] + [whole] * (5 + len(near) + len(far)),
        out_specs=[whole] * len(shapes),
        out_shape=shaped(shapes),
        compiler_params=pltpu.CompilerParams(vmem_limit_bytes=16 * 1024 * 1024),
        cost_estimate=pl.CostEstimate(flops=2**30, bytes_accessed=2**23, transcendentals=0),
        name="prepare",
    )(place, tokens, *near, *far, *known)


def train_kernel(
    rank,
    owned,
    tokens,
    labels,
    byte_full,
    out_full,
    byte_mixed,
    logit_gram,
    grams,
    normed_gram,
    inverse,
    squares,
    deltas,
    loss_out,
    work,
):
    vocab, depth = byte_full.shape
    count = tokens.shape[1]
    step = LANES // rank
    rows = depth * rank // LANES
    inner = depth // step
    chunks = depth // LANES
    onehot = (lax.broadcasted_iota(jnp.int32, (vocab, count), 0) == tokens[...]).astype(F32)
    label = (lax.broadcasted_iota(jnp.int32, (vocab, count), 0) == labels[...]).astype(F32)
    scale = inverse[...]
    a_t = owned[:rows, :].astype(F32).T.astype(BF16)
    table_a = jnp.zeros((rank, vocab), F32)
    for j in range(step):
        table_a += dot(a_t[j * rank : (j + 1) * rank, :], byte_mixed[:, j * inner : (j + 1) * inner], NT)
    work[...] = owned[rows:, :].astype(F32)
    b = jnp.concatenate([work[pl.ds(k, rank, stride=chunks), :] for k in range(chunks)], axis=1).astype(BF16)
    out_b = dot(b, out_full[...], NT)
    byte_b = dot(b, byte_full[...], NT)
    gram_b = dot(b, b, NT)
    low = exact(table_a, onehot, NN) * scale
    in_b = exact(byte_b, onehot, NN)
    s = 1.0 / (depth * rank) ** 0.5
    c = 4.0 / depth**0.5

    def one_step(low, both_b, gram_b):
        out_b, in_b = both_b[:, :vocab], both_b[:, vocab:]
        low_gram = small(gram_b, low)
        mean = (squares[...] + jnp.sum(low * (2.0 * s * in_b + (s * s) * low_gram), axis=0, keepdims=True)) / depth
        r = lax.rsqrt(jnp.maximum(mean, 0.0) + EPSILON)
        raw = logit_gram[...] + s * fine(out_b, low, TN)
        logits = raw * (c * r)
        top = jnp.max(logits, axis=0, keepdims=True)
        grown = jnp.exp(logits - top)
        total = jnp.sum(grown, axis=0, keepdims=True)
        loss = jnp.log(total) + top - jnp.sum(label * logits, axis=0, keepdims=True)
        error = grown / total - label
        k = (c / depth) * (r * r * r) * jnp.sum(error * raw, axis=0, keepdims=True)
        error = error * (c * r)
        d_low = s * (fine(out_b, error, NN) - k * (in_b + s * low_gram))
        kept = k * low
        on_both = rate * jnp.concatenate([-fine(low, error, NT), kept], axis=1)
        return loss, d_low, on_both, (rate * s) * fine(kept, low, NT)

    rate = learn_rate * s
    both_b = jnp.concatenate([out_b, in_b], axis=1)
    loss, d_low, on_both, more = one_step(low, both_b, gram_b)
    low_1 = low - learn_rate * fine(d_low, normed_gram[...], NN)
    both_b1 = both_b + small(more, both_b) + fine(on_both, grams[...], NN)
    gram_1 = gram_b + small(more, gram_b) + fine(on_both, both_b, NT)
    gram_b1 = gram_1 + small(gram_1, more.T) + fine(both_b1, on_both, NT)
    _, d_low1, on_both1, more1 = one_step(low_1, both_b1, gram_b1)
    total_b = more + more1 + small(more1, more)
    total_both = on_both + on_both1 + small(more1, on_both)
    total_out, total_in = total_both[:, :vocab], total_both[:, vocab:]
    on_byte = exact(total_in, onehot, NT)
    on_a = exact((-learn_rate) * scale * (d_low + d_low1), onehot, NT).astype(BF16)
    pieces = [dot(on_a, byte_mixed[:, j * inner : (j + 1) * inner], NN) for j in range(step)]
    deltas[:rows, :] = jnp.concatenate(pieces, axis=0).T.astype(BF16)
    delta_b = dot(total_b.astype(BF16), b, NN) + dot(total_out.astype(BF16), out_full[...], NN) + dot(on_byte.astype(BF16), byte_full[...], NN)
    for k in range(chunks):
        work[pl.ds(k, rank, stride=chunks), :] = delta_b[:, k * LANES : (k + 1) * LANES]
    deltas[rows:, :] = work[...].astype(BF16)
    loss_out[...] = jnp.broadcast_to(jnp.sum(loss, axis=1, keepdims=True) / count, loss_out.shape)


def train(rank, owned, tokens, labels, prepared):
    whole = pl.BlockSpec(memory_space=pltpu.VMEM)
    return pl.pallas_call(
        functools.partial(train_kernel, rank),
        in_specs=[whole] * (3 + len(prepared)),
        out_specs=[whole, whole],
        out_shape=[jax.ShapeDtypeStruct(owned.shape, BF16), jax.ShapeDtypeStruct((1, LANES), F32)],
        scratch_shapes=[pltpu.VMEM((owned.shape[0] // 2, LANES), F32)],
        compiler_params=pltpu.CompilerParams(vmem_limit_bytes=16 * 1024 * 1024),
        cost_estimate=pl.CostEstimate(flops=2**31, bytes_accessed=2**23, transcendentals=2**17),
        name="train",
    )(owned, tokens, labels, *prepared)


def stacked(parts):
    return jnp.concatenate([part[...].astype(F32) for part in parts], axis=0).astype(BF16)


def back_kernel(width, w, *refs):
    parts, out, held, sems = refs[:-3], refs[-3], refs[-2], refs[-1]
    slots = held.shape[0]
    blocks = w.shape[1] // width

    def copy(index):
        return pltpu.make_async_copy(w.at[:, span(index, width)], held.at[index % slots], sems.at[index % slots])

    @pl.loop(0, slots)
    def _(index):
        copy(index).start()

    out[...] = jnp.zeros_like(out)

    @pl.loop(0, blocks)
    def _(index):
        piece = stacked([part.at[:, span(index, width)] for part in parts])
        copy(index).wait()
        out[...] += dot(piece, held[index % slots], NT)

        @pl.when(index + slots < blocks)
        def _():
            copy(index + slots).start()


def back(w, parts):
    depth, columns = w.shape
    rows = sum(part.shape[0] for part in parts)
    width = min(2048, columns)
    slots = min(4, columns // width)
    whole = pl.BlockSpec(memory_space=pltpu.VMEM)
    return pl.pallas_call(
        functools.partial(back_kernel, width),
        in_specs=[pl.BlockSpec(memory_space=pltpu.HBM)] + [whole] * len(parts),
        out_specs=whole,
        out_shape=jax.ShapeDtypeStruct((rows, depth), F32),
        scratch_shapes=[pltpu.VMEM((slots, depth, width), BF16), pltpu.SemaphoreType.DMA((slots,))],
        compiler_params=pltpu.CompilerParams(vmem_limit_bytes=40 * 1024 * 1024),
        cost_estimate=pl.CostEstimate(flops=16 * rows * depth * columns, bytes_accessed=2 * depth * columns, transcendentals=0),
        name="hidden_back",
    )(w, *parts)


def grad_kernel(width, first, count, hidden_t, *refs):
    parts = refs[:-3] if first == 0 else refs[:-4]
    out, held, sems = refs[-3:]
    slots, depth, _ = held.shape
    bands = sems.shape[1]
    tall = depth // bands

    def copy(index, band):
        slot, rows = index % slots, pl.ds(band * tall, tall)
        return pltpu.make_async_copy(held.at[slot, rows], out.at[rows, span(first + index, width)], sems.at[slot, band])

    @pl.loop(0, count)
    def _(index):
        piece = stacked([part.at[:, span(first + index, width)] for part in parts])

        @pl.when(index >= slots)
        def _():
            for band in range(bands):
                copy(index - slots, band).wait()

        for band in range(bands):
            rows = pl.ds(band * tall, tall)
            held[index % slots, rows, :] = dot(hidden_t[rows, :], piece, NN).astype(BF16)
            copy(index, band).start()

    @pl.loop(max(0, count - slots), count)
    def _(index):
        for band in range(bands):
            copy(index, band).wait()


def grad(hidden_t, parts, calls):
    depth, rows = hidden_t.shape
    columns = parts[0].shape[1]
    width = min(1024, columns // 4)
    blocks = columns // width
    edges = [blocks * call // calls for call in range(calls + 1)]
    whole = pl.BlockSpec(memory_space=pltpu.VMEM)
    anywhere = pl.BlockSpec(memory_space=pltpu.HBM)
    out = None
    for call in range(calls):
        later = call > 0
        count = edges[call + 1] - edges[call]
        out = pl.pallas_call(
            functools.partial(grad_kernel, width, edges[call], count),
            in_specs=[whole] * (1 + len(parts)) + [anywhere] * later,
            out_specs=anywhere,
            out_shape=jax.ShapeDtypeStruct((depth, columns), BF16),
            scratch_shapes=[pltpu.VMEM((min(4, count), depth, width), BF16), pltpu.SemaphoreType.DMA((min(4, count), 2))],
            input_output_aliases={1 + len(parts): 0} if later else {},
            compiler_params=pltpu.CompilerParams(vmem_limit_bytes=16 * 1024 * 1024),
            cost_estimate=pl.CostEstimate(flops=16 * rows * depth * width * count, bytes_accessed=2 * depth * width * count, transcendentals=0),
            name="head_grad",
        )(hidden_t, *parts, *([out] if later else []))
    return out


def input_kernel(chosen_t, preact, mine, other, out):
    value = jnp.where(preact[...] > 0, mine[...] + other[...].astype(F32), 0.0)
    high = value.astype(BF16)
    low = (value - high.astype(F32)).astype(BF16)
    out[...] = dot(chosen_t[...], high, NN) + dot(chosen_t[...], low, NN)


def input_grad(chosen_t, preact, mine, other):
    whole = pl.BlockSpec(memory_space=pltpu.VMEM)
    return pl.pallas_call(
        input_kernel,
        in_specs=[whole] * 4,
        out_specs=whole,
        out_shape=jax.ShapeDtypeStruct((chosen_t.shape[0], preact.shape[1]), F32),
        compiler_params=pltpu.CompilerParams(vmem_limit_bytes=8 * 1024 * 1024),
        name="in_grad",
    )(chosen_t, preact, mine, other)


def swap(value, axis, bit):
    size = lax.axis_size(axis)
    return lax.ppermute(value, axis, [(i, i ^ (1 << bit)) for i in range(size)])


def gathered(value, axis):
    parts = [value]
    for bit in reversed(range(bits_of(lax.axis_size(axis)))):
        parts = parts + [swap(part, axis, bit) for part in parts]
    return parts


def steps(client_ids, client_table, in_weight, in_bias, head_weight, tokens, labels, byte_table, out_table):
    head_count = lax.axis_size("head")
    group_count = lax.axis_size("client")
    columns = head_weight.shape[1]
    depth = byte_table.shape[1] * group_count
    rank = columns * head_count // (2 * depth)
    top = bits_of(group_count) - 1
    side = lax.axis_index("head") & 1
    place = jnp.stack([lax.axis_index("client"), side]).astype(jnp.int32)
    part = out_table.shape[0] // 2
    out_low, out_high, byte_low, byte_high = out_table[:part], out_table[part:], byte_table[:part], byte_table[part:]
    crossing = swap(jnp.where(side == 0, out_high, byte_high), "client", top)
    far = [swap(jnp.concatenate([out_low, byte_low]), "client", top)]
    near = [out_table, byte_table]
    for bit in range(top):
        near = near + [swap(value, "client", bit) for value in near]
    pairs, hidden_t, preact, chosen_t = forward(
        place, client_ids, client_table, in_weight, in_bias, head_weight, head_count, group_count, 2
    )
    crossing, pairs[0] = lax.optimization_barrier((crossing, pairs[0]))
    handed = swap(crossing, "head", 0)
    far, late = far + [crossing], [handed]
    for bit in range(top):
        far = far + [swap(value, "client", bit) for value in far]
        late = late + [swap(value, "client", bit) for value in late]
    far = [value for at in range(1 << top) for value in (*far[2 * at : 2 * at + 2], late[at])]
    prepared = prepare(place, tokens, near, far, LANES // rank)
    halves = []
    for keep, send in pairs:
        got = swap(send, "client", 0)
        total = keep + got.astype(F32)
        for bit in range(1, top + 1):
            half = total.shape[0] // 2
            got = swap(total[half:].astype(BF16), "client", bit)
            total = total[:half] + got.astype(F32)
        halves.append(total.astype(BF16).reshape(head_count, -1, LANES))
    own = jnp.concatenate(halves, axis=1)
    own, prepared = lax.optimization_barrier((own, prepared))
    owned = lax.all_to_all(own, "head", split_axis=0, concat_axis=0, tiled=True)
    deltas, losses = train(rank, owned.reshape(-1, LANES), tokens, labels, prepared)
    returned = lax.all_to_all(deltas.reshape(own.shape), "head", split_axis=0, concat_axis=0, tiled=True)
    parts = gathered(returned.reshape(head_count, columns), "client")
    hidden_back = back(head_weight, parts)
    head_grad = grad(hidden_t, parts, 3)
    bits = bits_of(head_count)
    for bit in range(bits - 1):
        hidden_back = hidden_back + swap(hidden_back.astype(BF16), "head", bit).astype(F32)
    other = swap(hidden_back.astype(BF16), "head", bits - 1)
    in_grad = input_grad(chosen_t, preact, hidden_back, other)
    return head_grad, in_grad, losses[0, :1]


def solution(mesh):
    placed = (
        P(),
        P(),
        P(None, "client"),
        P("client"),
        P("client", "head"),
        P(("head", "client"), None),
        P(("head", "client"), None),
        P(None, "client"),
        P(None, "client"),
    )
    return jax.shard_map(
        steps,
        mesh=mesh,
        in_specs=placed,
        out_specs=(P("client", "head"), P(None, "client"), P(("head", "client"))),
        check_vma=False,
    )
```
